64 devices in a mesh: dp: 4 (over x, y), tp: 16 (over z, core).
Axes of the slice: x: 2, y: 2, z: 8, core: 2. Of those that a mesh axis runs over, the one named last changes fastest.
The devices are a block of a 4x4x8 slice.
Arguments:
- x_in: bfloat16 [4, 1024, 2048], P('dp', 'tp'), parts along dimension 0
- y_grad: bfloat16 [4, 1024, 2048], P('dp', 'tp'), parts along dimension 0
- ln_par: float32 [2, 4, 2048], replicated
- bias_d: float32 [2, 2, 2048], replicated
- w_qkv: bfloat16 [2, 2048, 3, 16, 128], P(None, None, None, 'tp')
- w_out: bfloat16 [2, 16, 128, 2048], P(None, 'tp')
- w_up: bfloat16 [2, 2048, 8192], P(None, None, 'tp')
- b_up: float32 [2, 8192], P(None, 'tp')
- w_down: bfloat16 [2, 8192, 2048], P(None, 'tp')
Outputs:
- output 1: bfloat16 [4, 1024, 2048], P('dp', 'tp'), parts along dimension 0
- output 2: bfloat16 [4, 1024, 2048], P('dp', 'tp'), parts along dimension 0
- output 3: float32 [8, 4, 2048], P('dp'), parts along dimension 0
- output 4: float32 [8, 2, 2048], P('dp'), parts along dimension 0
- output 5: bfloat16 [8, 2048, 3, 16, 128], P('dp', None, None, 'tp'), parts along dimension 0
- output 6: bfloat16 [8, 16, 128, 2048], P('dp', 'tp'), parts along dimension 0
- output 7: bfloat16 [8, 2048, 8192], P('dp', None, 'tp'), parts along dimension 0
- output 8: float32 [8, 8192], P('dp', 'tp'), parts along dimension 0
- output 9: bfloat16 [8, 8192, 2048], P('dp', 'tp'), parts along dimension 0
There are 4 independent parts. The reference program is written for one: setup_inputs(seed, part) draws one part's arguments, and reference() takes and returns one part's arrays. A program takes and returns all parts, laid end to end along the dimension named above; an argument that names none is the same for every part.
All inputs are finite; a program needn't handle non-finite values.
Results may differ from the reference program's by a relative error of at most 0.02.
Values are sent between devices in bfloat16 or wider.
A program may use at most 768 MiB of HBM per device.

```python
import math
import jax
import jax.numpy as jnp
from jax import lax

N_BATCH = 1
SEQ_LEN = 1024
D_MODEL = 2048
N_HEADS = 16
HEAD_DIM = 128
FF_DIM = 8192
N_LAYERS = 2


def layer_norm(row_vals, ln_gain, ln_shift):
    mean_val = jnp.mean(row_vals, axis=-1, keepdims=True)
    centered = row_vals - mean_val
    var_val = jnp.mean(centered * centered, axis=-1, keepdims=True)
    return centered * lax.rsqrt(var_val + 1e-5) * ln_gain + ln_shift


def setup_inputs(seed: int = 0, part: int = 0) -> dict:
    part_key = jax.random.fold_in(jax.random.key(seed), part)
    part_list = jax.random.split(part_key, 3)
    key_list = jax.random.split(jax.random.key(seed + 1), 7)
    act_shape = (N_BATCH, SEQ_LEN, D_MODEL)
    token_scale = jax.random.uniform(part_list[0], (N_BATCH, SEQ_LEN, 1), jnp.float32, 0.5, 1.5)
    x_in = (jax.random.normal(part_list[1], act_shape, jnp.float32) * token_scale).astype(jnp.bfloat16)
    y_grad = jax.random.normal(part_list[2], act_shape, jnp.float32).astype(jnp.bfloat16)
    ln_base = jnp.array([1.0, 0.0, 1.0, 0.0], jnp.float32)[None, :, None]
    ln_par = ln_base + 0.2 * jax.random.normal(key_list[0], (N_LAYERS, 4, D_MODEL), jnp.float32)
    bias_d = 0.2 * jax.random.normal(key_list[1], (N_LAYERS, 2, D_MODEL), jnp.float32)
    qk_gain = (math.log(SEQ_LEN) / 2.0) ** 0.25
    qkv_gain = jnp.array([qk_gain, qk_gain, 1.0], jnp.float32)[None, None, :, None, None] * D_MODEL ** -0.5
    w_qkv = (jax.random.normal(key_list[2], (N_LAYERS, D_MODEL, 3, N_HEADS, HEAD_DIM), jnp.float32) * qkv_gain).astype(jnp.bfloat16)
    out_gain = 0.3 * SEQ_LEN ** 0.25 * D_MODEL ** -0.5
    w_out = (jax.random.normal(key_list[3], (N_LAYERS, N_HEADS, HEAD_DIM, D_MODEL), jnp.float32) * out_gain).astype(jnp.bfloat16)
    w_up = (jax.random.normal(key_list[4], (N_LAYERS, D_MODEL, FF_DIM), jnp.float32) * D_MODEL ** -0.5).astype(jnp.bfloat16)
    b_up = 0.5 * jax.random.normal(key_list[5], (N_LAYERS, FF_DIM), jnp.float32)
    w_down = (jax.random.normal(key_list[6], (N_LAYERS, FF_DIM, D_MODEL), jnp.float32) * FF_DIM ** -0.5).astype(jnp.bfloat16)
    return dict(x_in=x_in, y_grad=y_grad, ln_par=ln_par, bias_d=bias_d, w_qkv=w_qkv, w_out=w_out, w_up=w_up, b_up=b_up, w_down=w_down)


def head_attention(qkv_head):
    q_head = qkv_head[:, 0].astype(jnp.float32)
    k_head = qkv_head[:, 1].astype(jnp.float32)
    v_head = qkv_head[:, 2].astype(jnp.float32)
    scores = jnp.dot(q_head, k_head.T) * (HEAD_DIM ** -0.5)
    positions = jnp.arange(SEQ_LEN)
    causal = positions[:, None] >= positions[None, :]
    scores = jnp.where(causal, scores, -1e30)
    prob_bf = jax.nn.softmax(scores, axis=-1).astype(jnp.bfloat16)
    return jnp.dot(prob_bf.astype(jnp.float32), v_head).astype(jnp.bfloat16)


def attention_all(qkv_vals):
    per_head = jnp.transpose(qkv_vals, (0, 3, 1, 2, 4)).reshape(N_BATCH * N_HEADS, SEQ_LEN, 3, HEAD_DIM)
    head_out = lax.map(jax.checkpoint(head_attention), per_head)
    return jnp.transpose(head_out.reshape(N_BATCH, N_HEADS, SEQ_LEN, HEAD_DIM), (0, 2, 1, 3))


def block_forward(residual, layer_w):
    ln_vals, bias_vals, w_qkv, w_out, w_up, b_up, w_down = layer_w
    h_one = layer_norm(residual, ln_vals[0], ln_vals[1]).astype(jnp.bfloat16)
    qkv_vals = jnp.einsum('bsd,dche->bsche', h_one.astype(jnp.float32), w_qkv.astype(jnp.float32)).astype(jnp.bfloat16)
    attn_vals = attention_all(qkv_vals)
    attn_out = jnp.einsum('bshe,hed->bsd', attn_vals.astype(jnp.float32), w_out.astype(jnp.float32))
    residual = residual + attn_out + bias_vals[0]
    h_two = layer_norm(residual, ln_vals[2], ln_vals[3]).astype(jnp.bfloat16)
    pre_act = jnp.einsum('bsd,df->bsf', h_two.astype(jnp.float32), w_up.astype(jnp.float32)) + b_up
    act_vals = jax.nn.gelu(pre_act, approximate=True).astype(jnp.bfloat16)
    mlp_out = jnp.einsum('bsf,fd->bsd', act_vals.astype(jnp.float32), w_down.astype(jnp.float32))
    return residual + mlp_out + bias_vals[1]


def reference(x_in, y_grad, ln_par, bias_d, w_qkv, w_out, w_up, b_up, w_down):
    weights = (ln_par, bias_d, w_qkv, w_out, w_up, b_up, w_down)

    def forward(x_vals, layer_stack):
        def scan_body(residual, layer_w):
            return block_forward(residual, layer_w), None
        final_res, _ = lax.scan(scan_body, x_vals.astype(jnp.float32), layer_stack)
        return final_res

    final_res, pullback = jax.vjp(forward, x_in, weights)
    x_ct, w_ct = pullback(y_grad.astype(jnp.float32))
    return (final_res.astype(jnp.bfloat16), x_ct, w_ct[0], w_ct[1], w_ct[2], w_ct[3], w_ct[4], w_ct[5], w_ct[6])
```

```python
import functools

import jax
import jax.numpy as jnp
from jax import lax
from jax.experimental import pallas as pl
from jax.experimental.pallas import tpu as pltpu
from jax.sharding import PartitionSpec as P

F32 = jnp.float32
BF16 = jnp.bfloat16
MESH = pl.DeviceIdType.MESH


class Ring:
    def __init__(self, n):
        self.n = n
        self.nz = n // 2
        self.me = lax.axis_index('tp')
        self.z = self.me // 2
        self.c = lax.rem(self.me, 2)
        self.sib = self.me + 1 - 2 * self.c
        self.next = {1: lax.rem(self.me + 2, n), -1: lax.rem(self.me + n - 2, n)}

    def chip(self, off):
        return lax.rem(self.z + (off + self.nz), self.nz)

    def enter(self):
        bar = pltpu.get_barrier_semaphore()
        for dev in (self.next[1], self.next[-1], self.sib):
            pl.semaphore_signal(bar, inc=1, device_id={'tp': dev}, device_id_type=MESH)
        pl.semaphore_wait(bar, 3)


def remote(src, dst, send_sem, recv_sem, dev):
    return pltpu.make_async_remote_copy(src_ref=src, dst_ref=dst, send_sem=send_sem, recv_sem=recv_sem,
                                        device_id={'tp': dev}, device_id_type=MESH)


def gather_pieces(ring):
    far = ring.nz // 2
    out = []
    for k in range(far):
        for h in range(2):
            for d in (1, -1):
                if k < far - 1 or h == (0 if d == 1 else 1):
                    out.append((d, k, h))
    return out


def ring_gather(ring, own_ref, all_ref, send_sem, recv_sem, psend, precv, on_hop=None):
    rows = own_ref.shape[0]
    half = rows // 2
    far = ring.nz // 2

    def piece(off, core, h):
        return all_ref.at[ring.chip(off), pl.ds(pl.multiple_of(core * rows + h * half, half), half)]

    def forward(d, k, h):
        dst = piece(-d * k, ring.c, h)
        src = own_ref.at[pl.ds(h * half, half)] if k == 0 else dst
        return remote(src, dst, send_sem.at[(1 - d) // 2, k, h], recv_sem.at[(1 - d) // 2, k, h], ring.next[d])

    def arrival(d, k, h):
        ref = piece(-d * (k + 1), ring.c, h)
        return remote(ref, ref, send_sem.at[(1 - d) // 2, k, h], recv_sem.at[(1 - d) // 2, k, h], ring.next[d])

    def pair(d, k, h, core):
        ref = piece(-d * (k + 1), core, h)
        return remote(ref, ref, psend.at[(1 - d) // 2, k, h], precv.at[(1 - d) // 2, k, h], ring.sib)

    def own_pair(core):
        ref = all_ref.at[ring.z, pl.ds(pl.multiple_of(core * rows, rows), rows)]
        return remote(own_ref, ref, psend.at[0, far, 0], precv.at[0, far, 0], ring.sib)

    order = gather_pieces(ring)
    for h in range(2):
        for d in (1, -1):
            forward(d, 0, h).start()
    own_pair(ring.c).start()
    all_ref[ring.z, pl.ds(pl.multiple_of(ring.c * rows, rows), rows)] = own_ref[...]
    own_pair(1 - ring.c).wait_recv()
    if on_hop is not None:
        on_hop((0,))
    for k in range(far):
        mine = [p for p in order if p[1] == k]
        for d, _, h in mine:
            arrival(d, k, h).wait_recv()
            if (d, k + 1, h) in order:
                forward(d, k + 1, h).start()
            pair(d, k, h, ring.c).start()
        for d, _, h in mine:
            pair(d, k, h, 1 - ring.c).wait_recv()
        if on_hop is not None:
            on_hop((k + 1, -(k + 1)) if k < far - 1 else (far,))
    for d, k, h in order:
        forward(d, k, h).wait_send()
        pair(d, k, h, ring.c).wait_send()
    own_pair(ring.c).wait_send()


def scatter_offsets(ring):
    far = ring.nz // 2
    offs = [far]
    for k in range(far - 1, 0, -1):
        offs += [k, -k]
    return offs + [0]


def ring_scatter(ring, own_part, give_ref, pair_ref, send_ref, recv_ref, send_sem, recv_sem, psend, precv, make=None):
    far = ring.nz // 2
    offs = scatter_offsets(ring)
    half = recv_ref.shape[2]
    slots = {}
    for d in (1, -1):
        hd = 0 if d == 1 else 1
        lst = [(far, hd)]
        for k in range(far - 1, 0, -1):
            lst += [(k, 1 - hd), (k, hd)]
        slots[d] = lst

    def pair(j):
        return remote(give_ref(j), pair_ref.at[j], psend.at[j], precv.at[j], ring.sib)

    def hop(d, s):
        i = (1 - d) // 2
        return remote(send_ref.at[i, s], recv_ref.at[i, s], send_sem.at[i, s], recv_sem.at[i, s], ring.next[d])

    made = set()

    def need(j):
        while len(made) <= j:
            i = len(made)
            if make is not None:
                make(i, offs[i])
            pair(i).start()
            made.add(i)

    paired = set()

    def base(j, h):
        need(min(j + 2, len(offs) - 1))
        if j not in paired:
            pair(j).wait_recv()
            paired.add(j)
        return own_part(j, h) + pair_ref[j, pl.ds(h * half, half)].astype(F32)

    need(0)
    for s in range(len(slots[1])):
        for d in (1, -1):
            k, h = slots[d][s]
            val = base(offs.index(d * k if k < far else far), h)
            if s >= 2:
                hop(d, s - 2).wait_recv()
                val = val + recv_ref[(1 - d) // 2, s - 2].astype(F32)
            send_ref[(1 - d) // 2, s] = val.astype(BF16)
            hop(d, s).start()
    last = len(slots[1])
    got = set()

    def total(h):
        val = base(len(offs) - 1, h)
        for d in (1, -1):
            s = last - 1 if slots[d][last - 1][1] == h else last - 2
            if (d, s) not in got:
                hop(d, s).wait_recv()
                got.add((d, s))
            val = val + recv_ref[(1 - d) // 2, s].astype(F32)
        return val

    def finish():
        for d in (1, -1):
            for s in range(last):
                hop(d, s).wait_send()
        for j in range(len(offs)):
            pair(j).wait_send()

    return total, finish


def gather_sems(n):
    far = n // 4
    return [pltpu.SemaphoreType.DMA((2, far + 1, 2)) for _ in range(4)]


def scatter_sems(n):
    steps = n // 2 - 1
    return [pltpu.SemaphoreType.DMA((2, steps)), pltpu.SemaphoreType.DMA((2, steps)),
            pltpu.SemaphoreType.DMA((n // 2,)), pltpu.SemaphoreType.DMA((n // 2,))]


VM = pl.BlockSpec(memory_space=pltpu.VMEM)


def comm_params(cid):
    return pltpu.CompilerParams(collective_id=cid, has_side_effects=True, vmem_limit_bytes=60 * 1024 * 1024)


def gather_rows(local, n):
    rows, width = local.shape

    def body(own_ref, all_ref, *sems):
        ring = Ring(n)
        ring.enter()
        ring_gather(ring, own_ref, all_ref, *sems)

    out = pl.pallas_call(
        body, out_shape=jax.ShapeDtypeStruct((n // 2, 2 * rows, width), BF16), in_specs=[VM], out_specs=VM,
        scratch_shapes=gather_sems(n), compiler_params=comm_params(1), name='ring_gather')(local)
    return out.reshape(n * rows, width)


def scatter_rows(partial, n):
    total_rows, width = partial.shape
    rows = total_rows // n
    half = rows // 2
    parts = partial.astype(BF16).reshape(n // 2, 2 * rows, width)

    def body(part_ref, out_ref, pair_ref, send_ref, recv_ref, *sems):
        ring = Ring(n)
        offs = scatter_offsets(ring)
        ring.enter()

        def own_part(j, h):
            at = pl.multiple_of(ring.c * rows + h * half, half)
            return part_ref[ring.chip(offs[j]), pl.ds(at, half)].astype(F32)

        def give(j):
            return part_ref.at[ring.chip(offs[j]), pl.ds(pl.multiple_of((1 - ring.c) * rows, rows), rows)]

        total, finish = ring_scatter(ring, own_part, give, pair_ref, send_ref, recv_ref, *sems)
        for h in range(2):
            out_ref[pl.ds(h * half, half)] = total(h)
        finish()

    steps = n // 2 - 1
    return pl.pallas_call(
        body, out_shape=jax.ShapeDtypeStruct((rows, width), F32), in_specs=[VM], out_specs=VM,
        scratch_shapes=[pltpu.VMEM((n // 2, rows, width), BF16), pltpu.VMEM((2, steps, half, width), BF16),
                        pltpu.VMEM((2, steps, half, width), BF16)] + scatter_sems(n),
        compiler_params=comm_params(2), name='ring_scatter')(parts)


def sum_small(vals, n):
    r, width = vals.shape
    cols = width // n
    pad = -r % 8
    blocks = jnp.pad(vals, ((0, pad), (0, 0))).reshape(r + pad, n, cols).transpose(1, 0, 2)

    def body(in_ref, out_ref, got_ref, s1, r1, s2, r2):
        me = lax.axis_index('tp')
        bar = pltpu.get_barrier_semaphore()
        peers = [lax.rem(me + j, n) for j in range(n)]
        for j in range(1, n):
            pl.semaphore_signal(bar, inc=1, device_id={'tp': peers[j]}, device_id_type=MESH)
        pl.semaphore_wait(bar, n - 1)
        first = [None] + [remote(in_ref.at[peers[j]], got_ref.at[j], s1.at[j], r1.at[j], peers[j]) for j in range(1, n)]
        for j in range(1, n):
            first[j].start()
        acc = in_ref[me]
        for j in range(1, n):
            first[j].wait_recv()
            acc = acc + got_ref[j]
        got_ref[0] = acc
        out_ref[me] = acc
        second = [None] + [remote(got_ref.at[0], out_ref.at[me], s2.at[j], r2.at[j], peers[j]) for j in range(1, n)]
        for j in range(1, n):
            second[j].start()
        for j in range(1, n):
            src = lax.rem(me + n - j, n)
            remote(got_ref.at[0], out_ref.at[src], s2.at[j], r2.at[j], peers[j]).wait_recv()
        for j in range(1, n):
            first[j].wait_send()
            second[j].wait_send()

    out = pl.pallas_call(
        body, out_shape=jax.ShapeDtypeStruct(blocks.shape, F32), in_specs=[VM], out_specs=VM,
        scratch_shapes=[pltpu.VMEM(blocks.shape, F32)] + [pltpu.SemaphoreType.DMA((n,))] * 4,
        compiler_params=comm_params(3), name='sum_small')(blocks)
    return out.transpose(1, 0, 2).reshape(r + pad, width)[:r]


def layer_norm(row_vals, ln_gain, ln_shift):
    mean_val = jnp.mean(row_vals, axis=-1, keepdims=True)
    centered = row_vals - mean_val
    var_val = jnp.mean(centered * centered, axis=-1, keepdims=True)
    return centered * lax.rsqrt(var_val + 1e-5) * ln_gain + ln_shift


def gelu_tanh(pre_act):
    return jax.nn.gelu(pre_act, approximate=True)


def mm(spec, a, b):
    return jnp.einsum(spec, a, b, preferred_element_type=F32)


def attention(q, k, v):
    seq_len = q.shape[0]
    scores = mm('qe,ke->qk', q, k) * q.shape[-1] ** -0.5
    positions = jnp.arange(seq_len)
    scores = jnp.where(positions[:, None] >= positions[None, :], scores, -1e30)
    prob = jax.nn.softmax(scores, axis=-1).astype(BF16)
    return mm('qk,ke->qe', prob, v).astype(BF16), prob


def attention_backward(d_attn, q, k, v, prob):
    d_prob = mm('qe,ke->qk', d_attn, v)
    d_v = mm('qk,qe->ke', prob, d_attn)
    row_dot = jnp.sum(d_prob * prob, axis=-1, keepdims=True)
    d_score = (prob * (d_prob - row_dot) * q.shape[-1] ** -0.5).astype(BF16)
    return mm('qk,ke->qe', d_score, k), mm('qk,qe->ke', d_score, q), d_v


def solution(mesh):
    n = mesh.shape['tp']

    def device_step(x_loc, dy_loc, ln_par, bias_d, w_qkv, w_out, w_up, b_up, w_down):
        n_layers = ln_par.shape[0]
        residual = x_loc[0].astype(F32)
        wq = jnp.transpose(w_qkv[:, :, :, 0], (0, 2, 1, 3))
        saved = []
        for l in range(n_layers):
            ln, bias = ln_par[l], bias_d[l]
            res_one = residual
            h_all = gather_rows(layer_norm(res_one, ln[0], ln[1]).astype(BF16), n)
            q, k, v = [mm('sd,de->se', h_all, wq[l, i]).astype(BF16) for i in range(3)]
            attn, prob = attention(q, k, v)
            res_two = res_one + scatter_rows(mm('se,ed->sd', attn, w_out[l, 0]), n) + bias[0]
            h2_all = gather_rows(layer_norm(res_two, ln[2], ln[3]).astype(BF16), n)
            pre_act = mm('sd,df->sf', h2_all, w_up[l]) + b_up[l]
            act_f, gelu_pull = jax.vjp(gelu_tanh, pre_act)
            act = act_f.astype(BF16)
            residual = res_two + scatter_rows(mm('sf,fd->sd', act, w_down[l]), n) + bias[1]
            saved.append((res_one, h_all, q, k, v, prob, attn, res_two, h2_all, gelu_pull, act))
        y_loc = residual.astype(BF16)

        d_res = dy_loc[0].astype(F32)
        grads = [None] * n_layers
        for l in reversed(range(n_layers)):
            res_one, h_all, q, k, v, prob, attn, res_two, h2_all, gelu_pull, act = saved[l]
            ln = ln_par[l]
            d_bias_two = jnp.sum(d_res, axis=0)
            d_all = gather_rows(d_res.astype(BF16), n)
            d_wdown = mm('sf,sd->fd', act, d_all)
            d_pre = gelu_pull(mm('sd,fd->sf', d_all, w_down[l]))[0]
            d_bup = jnp.sum(d_pre, axis=0)
            d_pre_bf = d_pre.astype(BF16)
            d_wup = mm('sd,sf->df', h2_all, d_pre_bf)
            d_h2 = scatter_rows(mm('sf,df->sd', d_pre_bf, w_up[l]), n)
            d_mid, d_g2, d_s2 = jax.vjp(layer_norm, res_two, ln[2], ln[3])[1](d_h2)
            d_res = d_res + d_mid
            d_bias_one = jnp.sum(d_res, axis=0)
            d_all = gather_rows(d_res.astype(BF16), n)
            d_wout = mm('se,sd->ed', attn, d_all)
            d_attn = mm('sd,ed->se', d_all, w_out[l, 0]).astype(BF16)
            d_proj = [g.astype(BF16) for g in attention_backward(d_attn, q, k, v, prob)]
            d_wqkv = jnp.stack([mm('sd,se->de', h_all, g) for g in d_proj], axis=0)
            d_h = scatter_rows(sum(mm('se,de->sd', d_proj[i], wq[l, i]) for i in range(3)), n)
            d_in, d_g1, d_s1 = jax.vjp(layer_norm, res_one, ln[0], ln[1])[1](d_h)
            d_res = d_res + d_in
            grads[l] = (jnp.stack([d_g1, d_s1, d_g2, d_s2, d_bias_one, d_bias_two]), d_wqkv, d_wout, d_wup, d_bup, d_wdown)
        small = sum_small(jnp.concatenate([g[0] for g in grads], axis=0), n)
        small = small.reshape(n_layers, 6, small.shape[-1])
        stacked = [jnp.stack([g[i] for g in grads]) for i in range(1, 6)]
        return (y_loc[None], d_res.astype(BF16)[None], small[:, :4], small[:, 4:],
                jnp.transpose(stacked[0].astype(BF16), (0, 2, 1, 3))[:, :, :, None], stacked[1].astype(BF16)[:, None],
                stacked[2].astype(BF16), stacked[3], stacked[4].astype(BF16))

    in_specs = (P('dp', 'tp', None), P('dp', 'tp', None), P(None, None, None), P(None, None, None),
                P(None, None, None, 'tp', None), P(None, 'tp', None, None), P(None, None, 'tp'), P(None, 'tp'), P(None, 'tp', None))
    out_specs = (P('dp', 'tp', None), P('dp', 'tp', None), P('dp', None, None), P('dp', None, None),
                 P('dp', None, None, 'tp', None), P('dp', 'tp', None, None), P('dp', None, 'tp'), P('dp', 'tp'), P('dp', 'tp', None))
    return jax.shard_map(device_step, mesh=mesh, in_specs=in_specs, out_specs=out_specs, check_vma=False)
```

```python
import math
import types

import jax
import jax.numpy as jnp
from jax import lax
from jax.experimental import pallas as pl
from jax.experimental.pallas import tpu as pltpu
from jax.sharding import PartitionSpec as P

F32 = jnp.float32
BF16 = jnp.bfloat16
MESH = pl.DeviceIdType.MESH


class Ring:
    def __init__(self, n):
        self.n = n
        self.nz = n // 2
        self.me = lax.axis_index('tp')
        self.z = self.me // 2
        self.c = lax.rem(self.me, 2)
        self.sib = self.me + 1 - 2 * self.c
        self.next = {1: lax.rem(self.me + 2, n), -1: lax.rem(self.me + n - 2, n)}

    def chip(self, off):
        return lax.rem(self.z + (off + self.nz), self.nz)

    def enter(self):
        bar = pltpu.get_barrier_semaphore()
        for dev in (self.next[1], self.next[-1], self.sib):
            pl.semaphore_signal(bar, inc=1, device_id={'tp': dev}, device_id_type=MESH)
        pl.semaphore_wait(bar, 3)


def remote(src, dst, send_sem, recv_sem, dev):
    return pltpu.make_async_remote_copy(src_ref=src, dst_ref=dst, send_sem=send_sem, recv_sem=recv_sem,
                                        device_id={'tp': dev}, device_id_type=MESH)


PIECES = 4


def side(d):
    return (1 - d) // 2


def piece_order(d):
    return list(range(PIECES)) if d == 1 else list(range(PIECES))[::-1]


def ring_gather(ring, own_ref, all_ref, send_sem, recv_sem, psend, precv, on_hop):
    rows = own_ref.shape[0]
    size = rows // PIECES
    far = ring.nz // 2

    def piece(off, core, q):
        return all_ref.at[ring.chip(off), pl.ds(pl.multiple_of(core * rows + q * size, size), size)]

    def moves(d, k):
        return piece_order(d)[:PIECES // 2] if k == far - 1 else piece_order(d)

    def forward(d, k, q):
        dst = piece(-d * k, ring.c, q)
        src = own_ref.at[pl.ds(q * size, size)] if k == 0 else dst
        return remote(src, dst, send_sem.at[side(d), k, q], recv_sem.at[side(d), k, q], ring.next[d])

    def arrival(d, k, q):
        ref = piece(-d * (k + 1), ring.c, q)
        return remote(ref, ref, send_sem.at[side(d), k, q], recv_sem.at[side(d), k, q], ring.next[d])

    def pair(d, k, q, core):
        ref = piece(-d * (k + 1), core, q)
        return remote(ref, ref, psend.at[side(d), k, q], precv.at[side(d), k, q], ring.sib)

    def own_pair(core):
        ref = all_ref.at[ring.z, pl.ds(pl.multiple_of(core * rows, rows), rows)]
        return remote(own_ref, ref, psend.at[0, far, 0], precv.at[0, far, 0], ring.sib)

    for i in range(PIECES):
        for d in (1, -1):
            forward(d, 0, piece_order(d)[i]).start()
    own_pair(ring.c).start()
    all_ref[ring.z, pl.ds(pl.multiple_of(ring.c * rows, rows), rows)] = own_ref[...]
    own_pair(1 - ring.c).wait_recv()
    on_hop((0,))
    for k in range(far):
        for i in range(len(moves(1, k))):
            for d in (1, -1):
                q = moves(d, k)[i]
                arrival(d, k, q).wait_recv()
                if k + 1 < far and q in moves(d, k + 1):
                    forward(d, k + 1, q).start()
                pair(d, k, q, ring.c).start()
        for d in (1, -1):
            for q in moves(d, k):
                pair(d, k, q, 1 - ring.c).wait_recv()
        on_hop((k + 1, -(k + 1)) if k < far - 1 else (far,))

    def finish():
        for d in (1, -1):
            for k in range(far):
                for q in moves(d, k):
                    forward(d, k, q).wait_send()
                    pair(d, k, q, ring.c).wait_send()
        own_pair(ring.c).wait_send()

    return finish


def ring_scatter(ring, part_ref, give_ref, pair_ref, send_ref, recv_ref, send_sem, recv_sem, psend, precv, make, work):
    far = ring.nz // 2
    rows = give_ref.shape[1]
    size = rows // PIECES
    offs = [far]
    for k in range(far - 1, 0, -1):
        offs += [k, -k]
    offs.append(0)
    work = list(work)
    slots = {}
    for d in (1, -1):
        first = piece_order(d)[:PIECES // 2]
        rest = piece_order(d)[PIECES // 2:]
        if d == -1:
            rest = rest[::-1]
            rest = rest[::-1]
        slots[d] = [(far, q) for q in first]
        for k in range(far - 1, 0, -1):
            slots[d] += [(k, q) for q in rest + first]
    steps = len(slots[1])

    def pair(j):
        return remote(give_ref.at[j], pair_ref.at[j], psend.at[j], precv.at[j], ring.sib)

    def hop(d, s):
        i = side(d)
        return remote(send_ref.at[i, s], recv_ref.at[i, s], send_sem.at[i, s], recv_sem.at[i, s], ring.next[d])

    made = []

    def need(j):
        while len(made) <= j:
            i = len(made)
            part_ref[i] = make(offs[i])
            give_ref[i] = part_ref[i, pl.ds(pl.multiple_of((1 - ring.c) * rows, rows), rows)].astype(BF16)
            pair(i).start()
            made.append(i)

    paired = set()

    def base(j, q):
        if j not in paired:
            pair(j).wait_recv()
            paired.add(j)
        at = pl.multiple_of(ring.c * rows + q * size, size)
        return part_ref[j, pl.ds(at, size)] + pair_ref[j, pl.ds(q * size, size)].astype(F32)

    need(2)
    for s in range(steps):
        for d in (1, -1):
            k, q = slots[d][s]
            val = base(offs.index(d * k if k < far else far), q)
            if s >= PIECES:
                hop(d, s - PIECES).wait_recv()
                val = val + recv_ref[side(d), s - PIECES].astype(F32)
            send_ref[side(d), s] = val.astype(BF16)
            hop(d, s).start()
        if len(made) < len(offs):
            need(len(made))
        elif work:
            work.pop(0)()
    for w in work:
        w()

    def total(q):
        val = base(len(offs) - 1, q)
        for d in (1, -1):
            s = slots[d].index((1, q))
            hop(d, s).wait_recv()
            val = val + recv_ref[side(d), s].astype(F32)
        return val

    def finish():
        for d in (1, -1):
            for s in range(steps):
                hop(d, s).wait_send()
        for j in range(len(offs)):
            pair(j).wait_send()

    return total, finish


VM = pl.BlockSpec(memory_space=pltpu.VMEM)
ANY = pl.BlockSpec(memory_space=pl.ANY)


def comm_params(cid):
    return pltpu.CompilerParams(collective_id=cid, has_side_effects=True, vmem_limit_bytes=62 * 1024 * 1024)


def sum_small(vals, n):
    r, width = vals.shape
    cols = width // n
    pad = -r % 8
    blocks = jnp.pad(vals, ((0, pad), (0, 0))).reshape(r + pad, n, cols).transpose(1, 0, 2)

    def body(in_ref, out_ref, got_ref, s1, r1, s2, r2):
        me = lax.axis_index('tp')
        bar = pltpu.get_barrier_semaphore()
        peers = [lax.rem(me + j, n) for j in range(n)]
        for j in range(1, n):
            pl.semaphore_signal(bar, inc=1, device_id={'tp': peers[j]}, device_id_type=MESH)
        pl.semaphore_wait(bar, n - 1)
        first = [None] + [remote(in_ref.at[peers[j]], got_ref.at[j], s1.at[j], r1.at[j], peers[j]) for j in range(1, n)]
        for j in range(1, n):
            first[j].start()
        acc = in_ref[me]
        for j in range(1, n):
            first[j].wait_recv()
            acc = acc + got_ref[j]
        got_ref[0] = acc
        out_ref[me] = acc
        second = [None] + [remote(got_ref.at[0], out_ref.at[me], s2.at[j], r2.at[j], peers[j]) for j in range(1, n)]
        for j in range(1, n):
            second[j].start()
        for j in range(1, n):
            src = lax.rem(me + n - j, n)
            remote(got_ref.at[0], out_ref.at[src], s2.at[j], r2.at[j], peers[j]).wait_recv()
        for j in range(1, n):
            first[j].wait_send()
            second[j].wait_send()

    out = pl.pallas_call(
        body, out_shape=jax.ShapeDtypeStruct(blocks.shape, F32), in_specs=[VM], out_specs=VM,
        scratch_shapes=[pltpu.VMEM(blocks.shape, F32)] + [pltpu.SemaphoreType.DMA((n,))] * 4,
        compiler_params=comm_params(1), name='sum_small')(blocks)
    return out.transpose(1, 0, 2).reshape(r + pad, width)[:r]


class Local:
    def __init__(self, sems):
        self.sems = sems
        self.used = 0
        self.out = []

    def start(self, src, dst):
        copy = pltpu.make_async_copy(src, dst, self.sems.at[self.used])
        self.used += 1
        copy.start()
        return copy

    def save(self, src, dst):
        self.out.append(self.start(src, dst))

    def finish(self):
        for copy in self.out:
            copy.wait()


def phase(name, cid, n, rows, width, inputs, outputs, scratch, body):
    nz = n // 2
    far = nz // 2
    size = rows // PIECES
    steps = PIECES * (far - 1) + PIECES // 2
    comm = {
        'all': pltpu.VMEM((nz, 2 * rows, width), BF16), 'part': pltpu.VMEM((nz, 2 * rows, width), F32),
        'give': pltpu.VMEM((nz, rows, width), BF16), 'pair': pltpu.VMEM((nz, rows, width), BF16),
        'send': pltpu.VMEM((2, steps, size, width), BF16), 'recv': pltpu.VMEM((2, steps, size, width), BF16),
        'g0': pltpu.SemaphoreType.DMA((2, far + 1, PIECES)), 'g1': pltpu.SemaphoreType.DMA((2, far + 1, PIECES)),
        'g2': pltpu.SemaphoreType.DMA((2, far + 1, PIECES)), 'g3': pltpu.SemaphoreType.DMA((2, far + 1, PIECES)),
        's0': pltpu.SemaphoreType.DMA((2, steps)), 's1': pltpu.SemaphoreType.DMA((2, steps)),
        's2': pltpu.SemaphoreType.DMA((nz,)), 's3': pltpu.SemaphoreType.DMA((nz,)),
        'local': pltpu.SemaphoreType.DMA((16,)),
    }
    own = {key: pltpu.VMEM(*val) for key, val in scratch.items()}
    names = list(inputs) + list(outputs) + list(comm) + list(own)

    def kernel(*refs):
        r = types.SimpleNamespace(**dict(zip(names, refs)))
        ring = Ring(n)
        local = Local(r.local)

        def gather(on_hop):
            ring.enter()
            return ring_gather(ring, r.own, r.all, r.g0, r.g1, r.g2, r.g3, on_hop)

        def scatter(make, work=()):
            return ring_scatter(ring, r.part, r.give, r.pair, r.send, r.recv, r.s0, r.s1, r.s2, r.s3, make, work)

        body(r, ring, local, gather, scatter)
        local.finish()

    out = pl.pallas_call(
        kernel, out_shape=[jax.ShapeDtypeStruct(s, t) for s, t, _ in outputs.values()],
        in_specs=[spec for _, spec in inputs.values()], out_specs=[spec for _, _, spec in outputs.values()],
        scratch_shapes=list(comm.values()) + list(own.values()), compiler_params=comm_params(cid), name=name,
    )(*[arr for arr, _ in inputs.values()])
    return types.SimpleNamespace(**dict(zip(outputs, out)))


def dot(a, b, ca=1, cb=0):
    return lax.dot_general(a, b, (((ca,), (cb,)), ((), ())), preferred_element_type=F32)


def layer_norm(row_vals, ln_gain, ln_shift):
    mean_val = jnp.mean(row_vals, axis=-1, keepdims=True)
    centered = row_vals - mean_val
    var_val = jnp.mean(centered * centered, axis=-1, keepdims=True)
    return centered * lax.rsqrt(var_val + 1e-5) * ln_gain + ln_shift


def layer_norm_back(d_out, row_vals, ln_gain):
    mean_val = jnp.mean(row_vals, axis=-1, keepdims=True)
    centered = row_vals - mean_val
    var_val = jnp.mean(centered * centered, axis=-1, keepdims=True)
    inv = lax.rsqrt(var_val + 1e-5)
    unit = centered * inv
    scaled = d_out * ln_gain
    pull = scaled - jnp.mean(scaled, axis=-1, keepdims=True) - unit * jnp.mean(scaled * unit, axis=-1, keepdims=True)
    return pull * inv, d_out * unit


GELU_C = math.sqrt(2.0 / math.pi)


def gelu(x):
    return x * (0.5 * (1.0 + jnp.tanh(GELU_C * (x + 0.044715 * (x * x * x)))))


def gelu_slope(x):
    t = jnp.tanh(GELU_C * (x + 0.044715 * (x * x * x)))
    return 0.5 * (1.0 + t) + 0.5 * x * (1.0 - t * t) * (GELU_C * (1.0 + 3 * 0.044715 * (x * x)))


def rows_of(ref, ring, offs):
    parts = [ref[ring.chip(o)] for o in offs]
    return parts[0] if len(parts) == 1 else jnp.concatenate(parts, axis=0)


def put_rows(ref, ring, offs, vals):
    m = ref.shape[1]
    for i, o in enumerate(offs):
        ref[ring.chip(o)] = vals[i * m:(i + 1) * m].astype(ref.dtype)


def flat(ref, cols=None):
    vals = ref[...] if cols is None else ref[:, :, cols]
    return vals.reshape(vals.shape[0] * vals.shape[1], vals.shape[2])


def forward_tail(r, total, bias, next_ln):
    size = r.own.shape[0] // PIECES
    for q in range(PIECES):
        at = pl.ds(q * size, size)
        res = r.res[at] + total(q) + bias
        r.res_out[at] = res
        r.own_out[at] = (res if next_ln is None else layer_norm(res, next_ln[0], next_ln[1])).astype(BF16)


def attention_forward(n, l, own, res, ln_par, bias_d, wq, w_out):
    rows, width = own.shape
    nz, e = n // 2, wq.shape[-1]
    blk = (nz, 2 * rows)

    def body(r, ring, local, gather, scatter):
        got_q = [local.start(r.wq.at[l, i], r.wq_v.at[:, pl.ds(i * e, e)]) for i in range(3)]
        got_o = local.start(r.wo.at[l], r.wo_v)

        def on_hop(offs):
            if offs == (0,):
                for g in got_q:
                    g.wait()
            vals = dot(rows_of(r.all, ring, offs), r.wq_v[...]).astype(BF16)
            for i, ref in enumerate((r.q, r.k, r.v)):
                put_rows(ref, ring, offs, vals[:, i * e:(i + 1) * e])

        done = gather(on_hop)
        got_o.wait()
        local.save(r.all, r.h_all)
        seq = nz * 2 * rows

        def make(off):
            chip = ring.chip(off)
            s = dot(r.q[chip], flat(r.k), 1, 1) * e ** -0.5
            row = lax.broadcasted_iota(jnp.int32, s.shape, 0) + chip * (2 * rows)
            col = lax.broadcasted_iota(jnp.int32, s.shape, 1)
            s = jnp.where(row >= col, s, -1e30)
            s = jnp.exp(s - jnp.max(s, axis=-1, keepdims=True))
            p = (s / jnp.sum(s, axis=-1, keepdims=True)).astype(BF16)
            r.prob_v[chip] = p
            a = dot(p, flat(r.v)).astype(BF16)
            r.attn[chip] = a
            return dot(a, r.wo_v[...])

        total, finish = scatter(make, [lambda: local.save(r.prob_v, r.prob)])
        forward_tail(r, total, r.bias[l, 0:1], (r.ln[l, 2:3], r.ln[l, 3:4]))
        done()
        finish()

    return phase(
        f'attn_fwd_{l}', 2 + l, n, rows, width,
        dict(own=(own, VM), res=(res, VM), ln=(ln_par, VM), bias=(bias_d, VM), wq=(wq, ANY), wo=(w_out, ANY)),
        dict(h_all=(blk + (width,), BF16, ANY), q=(blk + (e,), BF16, VM), k=(blk + (e,), BF16, VM), v=(blk + (e,), BF16, VM),
             prob=(blk + (nz * 2 * rows,), BF16, ANY), attn=(blk + (e,), BF16, VM),
             res_out=((rows, width), F32, VM), own_out=((rows, width), BF16, VM)),
        dict(wq_v=((width, 3 * e), BF16), wo_v=((e, width), BF16), prob_v=(blk + (nz * 2 * rows,), BF16)), body)


def mlp_forward(n, l, own, res, ln_par, bias_d, w_up, b_up, w_down):
    rows, width = own.shape
    nz, f = n // 2, w_up.shape[-1]
    blk = (nz, 2 * rows)
    last = l + 1 == ln_par.shape[0]

    def body(r, ring, local, gather, scatter):
        got_u = local.start(r.wu.at[l], r.wu_v)
        got_d = local.start(r.wd.at[l], r.wd_v)

        def on_hop(offs):
            if offs == (0,):
                got_u.wait()
            pre = dot(rows_of(r.all, ring, offs), r.wu_v[...]) + r.bup[l:l + 1]
            put_rows(r.pre_v, ring, offs, pre)
            put_rows(r.act_v, ring, offs, gelu(pre))

        done = gather(on_hop)
        got_d.wait()
        local.save(r.all, r.h_all)
        local.save(r.pre_v, r.pre)
        local.save(r.act_v, r.act)
        total, finish = scatter(lambda off: dot(r.act_v[ring.chip(off)], r.wd_v[...]))
        forward_tail(r, total, r.bias[l, 1:2], None if last else (r.ln[l + 1, 0:1], r.ln[l + 1, 1:2]))
        done()
        finish()

    return phase(
        f'mlp_fwd_{l}', 4 + l, n, rows, width,
        dict(own=(own, VM), res=(res, VM), ln=(ln_par, VM), bias=(bias_d, VM), wu=(w_up, ANY), bup=(b_up, VM), wd=(w_down, ANY)),
        dict(h_all=(blk + (width,), BF16, ANY), pre=(blk + (f,), F32, ANY), act=(blk + (f,), BF16, ANY),
             res_out=((rows, width), F32, VM), own_out=((rows, width), BF16, VM)),
        dict(wu_v=((width, f), BF16), wd_v=((f, width), BF16), pre_v=(blk + (f,), F32), act_v=(blk + (f,), BF16)), body)


def backward_tail(r, total, gain):
    size = r.own.shape[0] // PIECES
    d_gain = d_shift = d_bias = 0.0
    for q in range(PIECES):
        at = pl.ds(q * size, size)
        d_h = total(q)
        d_in, gain_terms = layer_norm_back(d_h, r.res[at], gain)
        d_gain = d_gain + jnp.sum(gain_terms, axis=0, keepdims=True)
        d_shift = d_shift + jnp.sum(d_h, axis=0, keepdims=True)
        d_old = r.d_res[at]
        d_bias = d_bias + jnp.sum(d_old, axis=0, keepdims=True)
        d_new = d_old + d_in
        r.d_res_out[at] = d_new
        r.own_out[at] = d_new.astype(BF16)
    r.small[0:1] = d_gain
    r.small[1:2] = d_shift
    r.small[2:3] = d_bias


def mlp_backward(n, l, own, d_res, res, ln_par, h_all, pre, act, w_up, w_down):
    rows, width = own.shape
    nz, f = n // 2, w_up.shape[-1]
    blk = (nz, 2 * rows)

    def body(r, ring, local, gather, scatter):
        got_d = local.start(r.wd.at[l], r.wd_v)
        got_p = local.start(r.pre, r.pre_v)
        got_u = local.start(r.wu.at[l], r.wu_v)
        got_a = local.start(r.act, r.act_v)
        got_h = local.start(r.h_all, r.h_v)
        sums = []

        def on_hop(offs):
            if offs == (0,):
                got_d.wait()
                got_p.wait()
            d_act = dot(rows_of(r.all, ring, offs), r.wd_v[...], 1, 1)
            d_pre = d_act * gelu_slope(rows_of(r.pre_v, ring, offs))
            sums.append(jnp.sum(d_pre, axis=0, keepdims=True))
            put_rows(r.d_pre, ring, offs, d_pre)

        done = gather(on_hop)
        r.d_bup[...] = sum(sums)
        got_u.wait()
        got_a.wait()
        got_h.wait()
        step = 256

        def down_part(i):
            cols = pl.ds(i * step, step)
            r.dwd_v[:, cols] = dot(flat(r.act_v), flat(r.all, cols), 0, 0).astype(BF16)

        def up_part(i):
            cols = pl.ds(i * step, step)
            r.dwu_v[cols] = dot(flat(r.h_v, cols), flat(r.d_pre), 0, 0).astype(BF16)

        work = [lambda i=i, g=g: g(i) for i in range(width // step) for g in (down_part, up_part)]
        total, finish = scatter(lambda off: dot(r.d_pre[ring.chip(off)], r.wu_v[...], 1, 1), work)
        local.save(r.dwd_v, r.dwd)
        local.save(r.dwu_v, r.dwu)
        backward_tail(r, total, r.ln[l, 2:3])
        done()
        finish()

    return phase(
        f'mlp_bwd_{l}', 6 + l, n, rows, width,
        dict(own=(own, VM), d_res=(d_res, VM), res=(res, VM), ln=(ln_par, VM), h_all=(h_all, ANY), pre=(pre, ANY), act=(act, ANY),
             wu=(w_up, ANY), wd=(w_down, ANY)),
        dict(dwu=((width, f), BF16, ANY), dwd=((f, width), BF16, ANY), d_bup=((1, f), F32, VM), small=((8, width), F32, VM),
             d_res_out=((rows, width), F32, VM), own_out=((rows, width), BF16, VM)),
        dict(wu_v=((width, f), BF16), wd_v=((f, width), BF16), pre_v=(blk + (f,), F32), act_v=(blk + (f,), BF16),
             h_v=(blk + (width,), BF16), d_pre=(blk + (f,), BF16), dwu_v=((width, f), BF16), dwd_v=((f, width), BF16)), body)


def attention_backward(n, l, own, d_res, res, ln_par, saved, wq, w_out):
    rows, width = own.shape
    nz, e = n // 2, wq.shape[-1]
    blk = (nz, 2 * rows)
    seq = nz * 2 * rows

    def body(r, ring, local, gather, scatter):
        got_o = local.start(r.wo.at[l], r.wo_v)
        got_p = local.start(r.prob, r.prob_v)
        got_q = [local.start(r.wq.at[l, i], r.wq_v.at[:, pl.ds(i * e, e)]) for i in range(3)]
        got_h = local.start(r.h_all, r.h_v)
        r.d_k[...] = jnp.zeros_like(r.d_k)
        r.d_v[...] = jnp.zeros_like(r.d_v)

        def on_hop(offs):
            if offs == (0,):
                got_o.wait()
                got_p.wait()
            d_attn = dot(rows_of(r.all, ring, offs), r.wo_v[...], 1, 1).astype(BF16)
            prob = rows_of(r.prob_v, ring, offs)
            d_prob = dot(d_attn, flat(r.v), 1, 1)
            row_dot = jnp.sum(d_prob * prob, axis=-1, keepdims=True)
            d_score = (prob * (d_prob - row_dot) * e ** -0.5).astype(BF16)
            d_q = dot(d_score, flat(r.k)).astype(BF16)
            for i, o in enumerate(offs):
                r.d_proj[ring.chip(o), :, 0:e] = d_q[i * 2 * rows:(i + 1) * 2 * rows]
            r.d_k[...] += dot(d_score, rows_of(r.q, ring, offs), 0, 0)
            r.d_v[...] += dot(prob, d_attn, 0, 0)

        done = gather(on_hop)
        r.d_proj[:, :, e:2 * e] = r.d_k[...].astype(BF16).reshape(blk + (e,))
        r.d_proj[:, :, 2 * e:] = r.d_v[...].astype(BF16).reshape(blk + (e,))
        for g in got_q:
            g.wait()
        got_h.wait()
        step = 256

        def out_part(i):
            cols = pl.ds(i * step, step)
            r.dwo[:, cols] = dot(flat(r.attn), flat(r.all, cols), 0, 0).astype(BF16)

        def proj_part(i):
            cols = pl.ds(i * step, step)
            vals = dot(flat(r.h_v, cols), flat(r.d_proj), 0, 0).astype(BF16)
            for j in range(3):
                r.dwq[j, cols] = vals[:, j * e:(j + 1) * e]

        work = [lambda i=i, g=g: g(i) for i in range(width // step) for g in (out_part, proj_part)]
        total, finish = scatter(lambda off: dot(r.d_proj[ring.chip(off)], r.wq_v[...], 1, 1), work)
        backward_tail(r, total, r.ln[l, 0:1])
        done()
        finish()

    s = saved
    return phase(
        f'attn_bwd_{l}', 8 + l, n, rows, width,
        dict(own=(own, VM), d_res=(d_res, VM), res=(res, VM), ln=(ln_par, VM), h_all=(s.h_all, ANY), q=(s.q, VM), k=(s.k, VM), v=(s.v, VM),
             prob=(s.prob, ANY), attn=(s.attn, VM), wq=(wq, ANY), wo=(w_out, ANY)),
        dict(dwq=((3, width, e), BF16, VM), dwo=((e, width), BF16, VM), small=((8, width), F32, VM),
             d_res_out=((rows, width), F32, VM), own_out=((rows, width), BF16, VM)),
        dict(wq_v=((width, 3 * e), BF16), wo_v=((e, width), BF16), prob_v=(blk + (seq,), BF16), h_v=(blk + (width,), BF16),
             d_proj=(blk + (3 * e,), BF16), d_k=((seq, e), F32), d_v=((seq, e), F32)), body)


def solution(mesh):
    n = mesh.shape['tp']

    def device_step(x_loc, dy_loc, ln_par, bias_d, w_qkv, w_out, w_up, b_up, w_down):
        n_layers = ln_par.shape[0]
        res = x_loc[0].astype(F32)
        wq = jnp.transpose(w_qkv[:, :, :, 0], (0, 2, 1, 3))
        wo = w_out[:, 0]
        own = layer_norm(res, ln_par[0, 0], ln_par[0, 1]).astype(BF16)
        saved = []
        for l in range(n_layers):
            att = attention_forward(n, l, own, res, ln_par, bias_d, wq, wo)
            mlp = mlp_forward(n, l, att.own_out, att.res_out, ln_par, bias_d, w_up, b_up, w_down)
            saved.append((res, att, mlp))
            own, res = mlp.own_out, mlp.res_out
        y_loc = own

        own, d_res = dy_loc[0], dy_loc[0].astype(F32)
        grads = [None] * n_layers
        for l in reversed(range(n_layers)):
            res_one, att, mlp = saved[l]
            b_mlp = mlp_backward(n, l, own, d_res, att.res_out, ln_par, mlp.h_all, mlp.pre, mlp.act, w_up, w_down)
            b_att = attention_backward(n, l, b_mlp.own_out, b_mlp.d_res_out, res_one, ln_par, att, wq, wo)
            own, d_res = b_att.own_out, b_att.d_res_out
            small = jnp.concatenate([b_att.small[:2], b_mlp.small[:2], b_att.small[2:3], b_mlp.small[2:3]])
            grads[l] = (small, b_att.dwq, b_att.dwo, b_mlp.dwu, b_mlp.d_bup[0], b_mlp.dwd)
        small = sum_small(jnp.concatenate([g[0] for g in grads], axis=0), n)
        small = small.reshape(n_layers, 6, small.shape[-1])
        stacked = [jnp.stack([g[i] for g in grads]) for i in range(1, 6)]
        return (y_loc[None], own[None], small[:, :4], small[:, 4:],
                jnp.transpose(stacked[0], (0, 2, 1, 3))[:, :, :, None], stacked[1][:, None],
                stacked[2], stacked[3], stacked[4])

    in_specs = (P('dp', 'tp', None), P('dp', 'tp', None), P(None, None, None), P(None, None, None),
                P(None, None, None, 'tp', None), P(None, 'tp', None, None), P(None, None, 'tp'), P(None, 'tp'), P(None, 'tp', None))
    out_specs = (P('dp', 'tp', None), P('dp', 'tp', None), P('dp', None, None), P('dp', None, None),
                 P('dp', None, None, 'tp', None), P('dp', 'tp', None, None), P('dp', None, 'tp'), P('dp', 'tp'), P('dp', 'tp', None))
    return jax.shard_map(device_step, mesh=mesh, in_specs=in_specs, out_specs=out_specs, check_vma=False)
```

```python
import math
import types

import jax
import jax.numpy as jnp
from jax import lax
from jax.experimental import pallas as pl
from jax.experimental.pallas import tpu as pltpu
from jax.sharding import PartitionSpec as P

F32 = jnp.float32
BF16 = jnp.bfloat16
MESH = pl.DeviceIdType.MESH
VM = pl.BlockSpec(memory_space=pltpu.VMEM)
ANY = pl.BlockSpec(memory_space=pl.ANY)
PIECES = 4
HELD = 5
FINAL = (2, 0, 3, 1)
GATHER = {1: ((2, 0, 3, 1), (2, 0, 3, 1)), -1: ((2, 0, 3, 1), (2, 3, 0, 1), (3, 2, 1, 0))}
GATHER_FAR = {1: (2, 0), -1: (3, 1)}
SCATTER_FAR = {1: (0, 1), -1: (2, 3)}
SCATTER = {1: (2, 3, 0, 1), -1: (0, 1, 2, 3)}
SCATTER_TWO = {1: (2, 3, 0, 1), -1: (0, 2, 1, 3)}


def side(d):
    return (1 - d) // 2


def remote(src, dst, send_sem, recv_sem, dev):
    return pltpu.make_async_remote_copy(src_ref=src, dst_ref=dst, send_sem=send_sem, recv_sem=recv_sem,
                                        device_id={'tp': dev}, device_id_type=MESH)


class Ring:
    def __init__(self, n):
        self.n = n
        self.nz = n // 2
        self.far = self.nz // 2
        self.me = lax.axis_index('tp')
        self.z = self.me // 2
        self.c = lax.rem(self.me, 2)
        self.sib = self.me + 1 - 2 * self.c
        self.next = {1: lax.rem(self.me + 2, n), -1: lax.rem(self.me + n - 2, n)}
        self.peers = [lax.rem(self.me + j, n) for j in range(n)]

    def chip(self, off):
        return lax.rem(self.z + (off + self.nz), self.nz)

    def enter(self, devices):
        bar = pltpu.get_barrier_semaphore()
        for dev in devices:
            pl.semaphore_signal(bar, inc=1, device_id={'tp': dev}, device_id_type=MESH)
        pl.semaphore_wait(bar, len(devices))


class Gather:
    def __init__(self, ring, own, land, sems):
        self.ring, self.own, self.land = ring, own, land
        self.sems = sems
        self.rows = own.shape[0]
        self.size = self.rows // PIECES

    def piece(self, off, core, q):
        return self.land.at[self.ring.chip(off), pl.ds(pl.multiple_of(core * self.rows + q * self.size, self.size), self.size)]

    def order(self, d, k):
        if k == self.ring.far - 1:
            return GATHER_FAR[d]
        return GATHER[d][min(k, len(GATHER[d]) - 1)]

    def forward(self, d, k, q):
        dst = self.piece(-d * k, self.ring.c, q)
        src = self.own.at[pl.ds(q * self.size, self.size)] if k == 0 else dst
        return remote(src, dst, self.sems[0].at[side(d), k, q], self.sems[1].at[side(d), k, q], self.ring.next[d])

    def arrival(self, d, k, q):
        ref = self.piece(-d * (k + 1), self.ring.c, q)
        return remote(ref, ref, self.sems[0].at[side(d), k, q], self.sems[1].at[side(d), k, q], self.ring.next[d])

    def pair(self, d, k, q, core):
        ref = self.piece(-d * (k + 1), core, q)
        return remote(ref, ref, self.sems[2].at[side(d), k, q], self.sems[3].at[side(d), k, q], self.ring.sib)

    def own_pair(self, q, core):
        far = self.ring.far
        return remote(self.own.at[pl.ds(q * self.size, self.size)], self.piece(0, core, q),
                      self.sems[2].at[0, far, q], self.sems[3].at[0, far, q], self.ring.sib)

    def launch(self, q):
        for d in (1, -1):
            self.forward(d, 0, q).start()
        self.own_pair(q, self.ring.c).start()

    def place_own(self):
        self.land[self.ring.z, pl.ds(pl.multiple_of(self.ring.c * self.rows, self.rows), self.rows)] = self.own[...]
        for q in range(PIECES):
            self.own_pair(q, 1 - self.ring.c).wait_recv()

    def hop(self, k):
        far = self.ring.far
        wait = {d: list(self.order(d, k + 1)) if k + 1 < far else [] for d in (1, -1)}
        have = {1: set(), -1: set()}
        for i in range(len(self.order(1, k))):
            for d in (1, -1):
                q = self.order(d, k)[i]
                self.arrival(d, k, q).wait_recv()
                have[d].add(q)
                while wait[d] and wait[d][0] in have[d]:
                    self.forward(d, k + 1, wait[d].pop(0)).start()
                self.pair(d, k, q, self.ring.c).start()

    def paired(self, k):
        for d in (1, -1):
            for q in self.order(d, k):
                self.pair(d, k, q, 1 - self.ring.c).wait_recv()

    def offs(self, k):
        return (k + 1, -(k + 1)) if k < self.ring.far - 1 else (self.ring.far,)

    def run(self, on_hop, middle):
        self.place_own()
        on_hop([self.ring.z], True)
        for k in range(self.ring.far):
            self.hop(k)
            if k == self.ring.far - 2:
                middle()
            self.paired(k)
            on_hop([self.ring.chip(o) for o in self.offs(k)], False)

    def settle(self):
        for d in (1, -1):
            for k in range(self.ring.far):
                for q in self.order(d, k):
                    self.forward(d, k, q).wait_send()
                    self.pair(d, k, q, self.ring.c).wait_send()
        for q in range(PIECES):
            self.own_pair(q, self.ring.c).wait_send()


class Scatter:
    def __init__(self, ring, part, give, pair, send, recv, sems):
        self.ring, self.part, self.give, self.pair_ref, self.send, self.recv = ring, part, give, pair, send, recv
        self.sems = sems
        self.rows = give.shape[1]
        self.size = self.rows // PIECES
        far = ring.far
        self.offs = [far]
        for k in range(far - 1, 0, -1):
            self.offs += [k, -k]
        self.offs.append(0)
        self.slots = {}
        for d in (1, -1):
            self.slots[d] = [(far, q) for q in SCATTER_FAR[d]]
            for k in range(far - 1, 0, -1):
                order = FINAL if k == 1 else SCATTER_TWO[d] if k == 2 else SCATTER[d]
                self.slots[d] += [(k, q) for q in order]
        self.steps = len(self.slots[1])
        self.paired = set()
        self.made = 0

    def pair(self, j):
        return remote(self.give.at[j], self.pair_ref.at[j], self.sems[2].at[j], self.sems[3].at[j], self.ring.sib)

    def hop(self, d, s):
        i = side(d)
        return remote(self.send.at[i, s], self.recv.at[i, s], self.sems[0].at[i, s], self.sems[1].at[i, s], self.ring.next[d])

    def fill(self, make):
        j = self.made
        self.part[j % HELD] = make(self.offs[j])
        theirs = pl.ds(pl.multiple_of((1 - self.ring.c) * self.rows, self.rows), self.rows)
        self.give[j] = self.part[j % HELD, theirs].astype(BF16)
        self.pair(j).start()
        self.made += 1

    def base(self, j, q):
        if j not in self.paired:
            self.pair(j).wait_recv()
            self.paired.add(j)
        at = pl.multiple_of(self.ring.c * self.rows + q * self.size, self.size)
        return self.part[j % HELD, pl.ds(at, self.size)] + self.pair_ref[j, pl.ds(q * self.size, self.size)].astype(F32)

    def run(self, make, work=None, count=0):
        n_off = len(self.offs)
        fill_after = {0: 2}
        for j in range(3, n_off):
            fill_after[min(2 * (j - 2), self.steps - PIECES - (n_off - 1 - j) - 1)] = j
        quiet = [s for s in range(self.steps - 1) if s not in fill_after]
        begun = 0
        self.fill(make)
        self.fill(make)
        for s in range(self.steps):
            for d in (1, -1):
                k, q = self.slots[d][s]
                val = self.base(self.offs.index(d * k if k < self.ring.far else self.ring.far), q)
                if (k + 1, q) in self.slots[d]:
                    t = self.slots[d].index((k + 1, q))
                    self.hop(d, t).wait_recv()
                    val = val + self.recv[side(d), t].astype(F32)
                self.send[side(d), s] = val.astype(BF16)
                self.hop(d, s).start()
            if s in fill_after:
                self.fill(make)
            elif s in quiet and begun < count:
                upto = begun + -(-(count - begun) // len([t for t in quiet if t >= s]))
                if upto - begun == 1:
                    work(begun)
                else:
                    pl.loop(begun, upto)(work)
                begun = upto

    def total(self, q):
        val = self.base(len(self.offs) - 1, q)
        for d in (1, -1):
            s = self.slots[d].index((1, q))
            self.hop(d, s).wait_recv()
            val = val + self.recv[side(d), s].astype(F32)
        return val

    def settle(self):
        for d in (1, -1):
            for s in range(self.steps):
                self.hop(d, s).wait_send()
        for j in range(len(self.offs)):
            self.pair(j).wait_send()


class Exchange:
    def __init__(self, ring, rows, got, out, sems):
        self.ring, self.rows, self.got, self.out = ring, rows, got, out
        self.sems = sems
        self.cols = rows.shape[1] // ring.n

    def block(self, ref, dev):
        return ref.at[:, pl.ds(pl.multiple_of(dev * self.cols, self.cols), self.cols)]

    def first(self, j):
        peer = self.ring.peers[j]
        return remote(self.block(self.rows, peer), self.got.at[j], self.sems[0].at[j], self.sems[1].at[j], peer)

    def second(self, j, dev):
        return remote(self.got.at[0], self.block(self.out, dev), self.sems[2].at[j], self.sems[3].at[j], self.ring.peers[j])

    def start(self):
        for j in range(1, self.ring.n):
            self.first(j).start()

    def add(self):
        mine = pl.ds(pl.multiple_of(self.ring.me * self.cols, self.cols), self.cols)
        acc = self.rows[:, mine]
        for j in range(1, self.ring.n):
            self.first(j).wait_recv()
            acc = acc + self.got[j]
        self.got[0] = acc
        self.out[:, mine] = acc
        for j in range(1, self.ring.n):
            self.second(j, self.ring.me).start()

    def finish(self):
        for j in range(1, self.ring.n):
            self.second(j, lax.rem(self.ring.me + self.ring.n - j, self.ring.n)).wait_recv()
        for j in range(1, self.ring.n):
            self.first(j).wait_send()
            self.second(j, self.ring.me).wait_send()


class Local:
    def __init__(self, sems):
        self.sems = sems
        self.used = 0

    def copies(self, *pairs):
        at = self.used
        self.used += len(pairs)

        def of(l):
            return [pltpu.make_async_copy(*pair(l), self.sems.at[at + i]) for i, pair in enumerate(pairs)]

        return types.SimpleNamespace(start=lambda l: [c.start() for c in of(l)], wait=lambda l: [c.wait() for c in of(l)])


def dot(a, b, ca=1, cb=0):
    return lax.dot_general(a, b, (((ca,), (cb,)), ((), ())), preferred_element_type=F32)


def layer_norm(row_vals, ln_gain, ln_shift):
    mean_val = jnp.mean(row_vals, axis=-1, keepdims=True)
    centered = row_vals - mean_val
    var_val = jnp.mean(centered * centered, axis=-1, keepdims=True)
    return centered * lax.rsqrt(var_val + 1e-5) * ln_gain + ln_shift


def layer_norm_back(d_out, row_vals, ln_gain):
    mean_val = jnp.mean(row_vals, axis=-1, keepdims=True)
    centered = row_vals - mean_val
    var_val = jnp.mean(centered * centered, axis=-1, keepdims=True)
    inv = lax.rsqrt(var_val + 1e-5)
    unit = centered * inv
    scaled = d_out * ln_gain
    pull = scaled - jnp.mean(scaled, axis=-1, keepdims=True) - unit * jnp.mean(scaled * unit, axis=-1, keepdims=True)
    return pull * inv, d_out * unit


GELU_C = math.sqrt(2.0 / math.pi)


def gelu(x):
    return x * (0.5 * (1.0 + jnp.tanh(GELU_C * (x + 0.044715 * (x * x * x)))))


def gelu_slope(x):
    t = jnp.tanh(GELU_C * (x + 0.044715 * (x * x * x)))
    return 0.5 * (1.0 + t) + 0.5 * x * (1.0 - t * t) * (GELU_C * (1.0 + 3 * 0.044715 * (x * x)))


def rows_of(ref, chips):
    parts = [ref[z] for z in chips]
    return parts[0] if len(parts) == 1 else jnp.concatenate(parts, axis=0)


def put_rows(ref, chips, vals):
    m = ref.shape[1]
    for i, z in enumerate(chips):
        ref[z] = vals[i * m:(i + 1) * m].astype(ref.dtype)


def flat(ref, cols=None):
    vals = ref[...] if cols is None else ref[:, :, cols]
    return vals.reshape(vals.shape[0] * vals.shape[1], vals.shape[2])


def col_sum(vals):
    return jnp.sum(vals, axis=0, keepdims=True)


def forward_kernel(r, n, n_layers):
    ring = Ring(n)
    local = Local(r.local)
    rows, width = r.dy.shape
    e = r.wq.shape[-1]
    size = rows // PIECES
    scale = e ** -0.5
    last = n_layers - 1
    gathers = [Gather(ring, own, r.all.at[i], [r.gs.at[i, t] for t in range(4)])
               for i, own in enumerate((r.own.at[0], r.own.at[1], r.dy))]

    def scatter_at(i):
        return Scatter(ring, r.part, r.give, r.pair.at[i], r.send, r.recv.at[i],
                       [r.ss.at[i, 0], r.ss.at[i, 1], r.ps.at[i, 0], r.ps.at[i, 1]])

    def piece(q):
        return pl.ds(q * size, size)

    attn_w = local.copies(*[lambda l, i=i: (r.wq.at[l, i], r.wq_v.at[:, pl.ds(i * e, e)]) for i in range(3)],
                          lambda l: (r.wo.at[l], r.wo_v))
    mlp_w = local.copies(lambda l: (r.wd.at[l], r.wd_v), lambda l: (r.wu.at[l], r.wu_v))
    dy = gathers[2]
    save_one = local.copies(lambda l: (r.all.at[0], r.h_one.at[l]), *[lambda l, a=a, b=b: (a.at[l], b.at[l]) for a, b in
                                                                      ((r.q, r.q_h), (r.k, r.k_h), (r.v, r.v_h))])
    save_attn = local.copies(lambda l: (r.prob, r.prob_h.at[l]), lambda l: (r.attn.at[l], r.attn_h.at[l]))
    save_mlp = local.copies(lambda l: (r.all.at[1], r.h_two.at[l]), lambda l: (r.pre, r.pre_h.at[l]),
                            lambda l: (r.act.at[l], r.act_h.at[l]))
    save_dy = local.copies(lambda l: (r.all.at[2], r.dy_all))

    attn_w.start(0)
    mlp_w.start(0)
    for q in FINAL:
        res = r.x[piece(q)].astype(F32)
        r.res[0, piece(q)] = res
        r.own[0, piece(q)] = layer_norm(res, r.ln[0, 0:1], r.ln[0, 1:2]).astype(BF16)
    ring.enter([ring.next[1], ring.next[-1], ring.sib])
    for q in FINAL:
        gathers[0].launch(q)

    def side_steps(phase, odd):
        def go():
            for k in range(odd, min(2 * n_layers, ring.far), 2):
                @pl.when(phase == k)
                def _():
                    if k == 0:
                        for q in FINAL:
                            dy.launch(q)
                    else:
                        dy.hop(k - 1)
        return go

    @pl.loop(0, n_layers)
    def forward(l):
        inner = l < last

        def on_attn(chips, first):
            if first:
                attn_w.wait(l)
            vals = dot(rows_of(r.all.at[0], chips), r.wq_v[...]).astype(BF16)
            for i, ref in enumerate((r.q, r.k, r.v)):
                put_rows(ref.at[l], chips, vals[:, i * e:(i + 1) * e])

        gathers[0].run(on_attn, side_steps(2 * l, 0))

        @pl.when(l > 0)
        def _():
            gathers[1].settle()
            scatter_at(1).settle()
            save_mlp.wait(l)

        save_one.start(l)

        def make(off):
            chip = ring.chip(off)
            s = dot(r.q[l, chip], flat(r.k.at[l]), 1, 1) * scale
            row = lax.broadcasted_iota(jnp.int32, s.shape, 0) + chip * (2 * rows)
            col = lax.broadcasted_iota(jnp.int32, s.shape, 1)
            s = jnp.where(row >= col, s, -1e30)
            s = jnp.exp(s - jnp.max(s, axis=-1, keepdims=True))
            p = (s / jnp.sum(s, axis=-1, keepdims=True)).astype(BF16)
            r.prob[chip] = p
            a = dot(p, flat(r.v.at[l])).astype(BF16)
            r.attn[l, chip] = a
            return dot(a, r.wo_v[...])

        sc = scatter_at(0)
        sc.run(make)
        for q in FINAL:
            res = r.res[2 * l, piece(q)] + sc.total(q) + r.bias[l, 0:1]
            r.res[2 * l + 1, piece(q)] = res
            r.own[1, piece(q)] = layer_norm(res, r.ln[l, 2:3], r.ln[l, 3:4]).astype(BF16)
            gathers[1].launch(q)
        save_attn.start(l)

        @pl.when(inner)
        def _():
            attn_w.start(l + 1)

        def on_mlp(chips, first):
            if first:
                mlp_w.wait(l)
            pre = dot(rows_of(r.all.at[1], chips), r.wu_v[...]) + r.bup[l]
            put_rows(r.pre, chips, pre)
            put_rows(r.act.at[l], chips, gelu(pre))

        gathers[1].run(on_mlp, side_steps(2 * l + 1, 1))
        gathers[0].settle()
        scatter_at(0).settle()
        save_one.wait(l)
        save_attn.wait(l)
        save_mlp.start(l)
        sc = scatter_at(1)
        sc.run(lambda off: dot(r.act[l, ring.chip(off)], r.wd_v[...]))
        for q in FINAL:
            res = r.res[2 * l + 1, piece(q)] + sc.total(q) + r.bias[l, 1:2]
            r.y[piece(q)] = res.astype(BF16)

            @pl.when(inner)
            def _():
                r.res[2 * l + 2, piece(q)] = res
                r.own[0, piece(q)] = layer_norm(res, r.ln[l + 1, 0:1], r.ln[l + 1, 1:2]).astype(BF16)
                gathers[0].launch(q)

        @pl.when(inner)
        def _():
            mlp_w.start(l + 1)

    for k in range(min(2 * n_layers, ring.far) - 1, ring.far):
        dy.hop(k)
    dy.place_own()
    for k in range(ring.far):
        dy.paired(k)

    save_dy.start(0)
    dy.settle()
    gathers[1].settle()
    scatter_at(1).settle()
    save_mlp.wait(last)
    save_dy.wait(0)


def backward_kernel(r, n, n_layers):
    ring = Ring(n)
    local = Local(r.local)
    rows, width = r.dy.shape
    e = r.wq.shape[-1]
    size = rows // PIECES
    scale = e ** -0.5
    last = n_layers - 1
    gathers = [Gather(ring, own, r.all.at[i], [r.gs.at[i, t] for t in range(4)])
               for i, own in enumerate((r.own.at[0], r.own.at[1]))]

    def scatter_at(i):
        return Scatter(ring, r.part, r.give, r.pair.at[i], r.send, r.recv.at[i],
                       [r.ss.at[i, 0], r.ss.at[i, 1], r.ps.at[i, 0], r.ps.at[i, 1]])

    def piece(q):
        return pl.ds(q * size, size)

    attn_w = local.copies(*[lambda l, i=i: (r.wq.at[l, i], r.wq_v.at[:, pl.ds(i * e, e)]) for i in range(3)],
                          lambda l: (r.wo.at[l], r.wo_v))
    mlp_w = local.copies(lambda l: (r.wd.at[l], r.wd_v), lambda l: (r.wu.at[l], r.wu_v))
    tile = 256
    blocks = width // tile
    load_one = local.copies(lambda l: (r.h_one.at[l], r.all.at[2]))
    load_two = local.copies(lambda l: (r.h_two.at[l], r.all.at[2]))
    load_top = local.copies(lambda l: (r.dy_all, r.all.at[2]))
    load_top_two = local.copies(lambda l: (r.h_two.at[l], r.all.at[1]))
    load_prob = local.copies(lambda l: (r.prob_h.at[l], r.prob))
    load_pre = local.copies(lambda l: (r.pre_h.at[l], r.pre))
    load_act = local.copies(lambda l: (r.act_h, r.act))
    load_attn = local.copies(*[lambda l, a=a, b=b: (a, b) for a, b in
                               ((r.q_h, r.q), (r.k_h, r.k), (r.v_h, r.v), (r.attn_h, r.attn))])
    save_dmlp = local.copies(lambda l: (r.dwd_v, r.dwd.at[l]), lambda l: (r.dwu_v, r.dwu.at[l]))
    save_dattn = local.copies(lambda l: (r.dwo_v, r.dwo.at[l]), lambda l: (r.dwq_v, r.dwq.at[l]))

    load_top.start(0)
    load_pre.start(last)
    mlp_w.start(last)
    load_top_two.start(last)
    load_act.start(0)
    attn_w.start(last)
    load_prob.start(last)
    load_attn.start(0)
    for q in FINAL:
        r.d_res[piece(q)] = r.dy[piece(q)].astype(F32)
    r.small_a[...] = jnp.zeros_like(r.small_a)
    r.small_b[...] = jnp.zeros_like(r.small_b)
    ring.enter(ring.peers[1:])

    def put_small(l, i, val):
        for m in range(n_layers):
            @pl.when(l == m)
            def _():
                if m == 0 and i < 2:
                    r.small_b[i:i + 1] = val
                else:
                    at = i - 2 if m == 0 else 6 * m - 2 + i
                    r.small_a[at:at + 1] = val

    def backward_tail(sc, res_at, gain, after, out):
        d_gain = d_shift = d_bias = 0.0
        for q in FINAL:
            d_h = sc.total(q)
            d_in, terms = layer_norm_back(d_h, r.res[res_at, piece(q)], gain)
            d_new = r.d_res[piece(q)] + d_in
            out(q, d_new)
            d_gain, d_shift, d_bias = d_gain + col_sum(terms), d_shift + col_sum(d_h), d_bias + col_sum(d_new)
            r.d_res[piece(q)] = d_new
        after(d_gain, d_shift, d_bias)

    put_small(last, 5, col_sum(r.d_res[...]))
    ex_a = Exchange(ring, r.small_a, r.got_a, r.sum_a, [r.es.at[0, t] for t in range(4)])
    ex_b = Exchange(ring, r.small_b, r.got_b, r.sum_b, [r.es.at[1, t] for t in range(4)])

    @pl.loop(0, n_layers)
    def backward(i):
        l = last - i
        top, lower = i == 0, i > 0
        at_d = 1 + (n_layers - i) // n_layers
        at_h = 3 - at_d

        @pl.when(lower)
        def _():
            load_two.start(l)
            load_prob.start(l)

        r.bup_sum[...] = jnp.zeros_like(r.bup_sum)

        def on_mlp(chips, first):
            if first:
                mlp_w.wait(l)
                load_pre.wait(l)
            d_act = dot(rows_of(r.all.at[at_d], chips), r.wd_v[...], 1, 1)
            d_pre = d_act * gelu_slope(rows_of(r.pre, chips))
            r.bup_sum[...] += col_sum(d_pre)
            put_rows(r.d_pre, chips, d_pre)

        @pl.when(lower)
        def _():
            gathers[1].run(on_mlp, lambda: None)
            gathers[0].settle()
            scatter_at(1).settle()
            save_dattn.wait(l)
            load_two.wait(l)

        @pl.when(top)
        def _():
            load_top.wait(0)
            load_pre.wait(l)
            mlp_w.wait(l)

            @pl.loop(0, ring.far)
            def _(z):
                on_mlp([z, z + ring.far], False)

            load_top_two.wait(l)
            load_act.wait(0)

        def mlp_work(j):
            cols = pl.ds(pl.multiple_of(j * tile, tile), tile)
            r.dwd_v[:, cols] = dot(flat(r.act.at[l]), flat(r.all.at[at_d], cols), 0, 0).astype(BF16)
            r.dwu_v[cols] = dot(flat(r.all.at[at_h], cols), flat(r.d_pre), 0, 0).astype(BF16)

        sc = scatter_at(0)
        sc.run(lambda off: dot(r.d_pre[ring.chip(off)], r.wu_v[...], 1, 1), mlp_work, blocks)
        save_dmlp.start(l)

        def hand_on(q, d_new):
            r.own[0, piece(q)] = d_new.astype(BF16)
            gathers[0].launch(q)

        def after_mlp(d_gain, d_shift, d_bias):
            put_small(l, 2, d_gain)
            put_small(l, 3, d_shift)
            put_small(l, 4, d_bias)
            for m in range(n_layers):
                @pl.when(l == m)
                def _():
                    r.d_bup[m:m + 1] = r.bup_sum[...]

        backward_tail(sc, 2 * l + 1, r.ln[l, 2:3], after_mlp, hand_on)

        @pl.when(l > 0)
        def _():
            load_pre.start(l - 1)
            mlp_w.start(l - 1)

        @pl.when(l == 0)
        def _():
            ex_a.start()

        load_one.start(l)
        r.d_k[...] = jnp.zeros_like(r.d_k)
        r.d_v[...] = jnp.zeros_like(r.d_v)

        def on_attn(chips, first):
            if first:
                attn_w.wait(l)
                load_prob.wait(l)

                @pl.when(top)
                def _():
                    load_attn.wait(0)
            d_attn = dot(rows_of(r.all.at[0], chips), r.wo_v[...], 1, 1).astype(BF16)
            prob = rows_of(r.prob, chips)
            d_prob = dot(d_attn, flat(r.v.at[l]), 1, 1)
            row_dot = jnp.sum(d_prob * prob, axis=-1, keepdims=True)
            d_score = (prob * (d_prob - row_dot) * scale).astype(BF16)
            d_q = dot(d_score, flat(r.k.at[l])).astype(BF16)
            for t, z in enumerate(chips):
                r.d_proj[z, :, 0:e] = d_q[t * 2 * rows:(t + 1) * 2 * rows]
            r.d_k[...] += dot(d_score, rows_of(r.q.at[l], chips), 0, 0)
            r.d_v[...] += dot(prob, d_attn, 0, 0)

        gathers[0].run(on_attn, lambda: None)

        @pl.when(lower)
        def _():
            gathers[1].settle()

        scatter_at(0).settle()
        save_dmlp.wait(l)
        load_one.wait(l)
        blk = r.d_proj.shape[:2] + (e,)
        r.d_proj[:, :, e:2 * e] = r.d_k[...].astype(BF16).reshape(blk)
        r.d_proj[:, :, 2 * e:] = r.d_v[...].astype(BF16).reshape(blk)

        def attn_work(j):
            cols = pl.ds(pl.multiple_of(j * tile, tile), tile)
            r.dwo_v[:, cols] = dot(flat(r.attn.at[l]), flat(r.all.at[0], cols), 0, 0).astype(BF16)
            vals = dot(flat(r.all.at[2], cols), flat(r.d_proj), 0, 0).astype(BF16)
            for t in range(3):
                r.dwq_v[t, cols] = vals[:, t * e:(t + 1) * e]

        sc = scatter_at(1)
        sc.run(lambda off: dot(r.d_proj[ring.chip(off)], r.wq_v[...], 1, 1), attn_work, blocks)
        save_dattn.start(l)

        @pl.when(l == 0)
        def _():
            ex_a.add()

        def out(q, d_new):
            r.dx[piece(q)] = d_new.astype(BF16)

            @pl.when(l > 0)
            def _():
                r.own[1, piece(q)] = d_new.astype(BF16)
                gathers[1].launch(q)

        def after_attn(d_gain, d_shift, d_bias):
            put_small(l, 0, d_gain)
            put_small(l, 1, d_shift)
            put_small(l - 1, 5, d_bias)

        backward_tail(sc, 2 * l, r.ln[l, 0:1], after_attn, out)

        @pl.when(l > 0)
        def _():
            attn_w.start(l - 1)

    ex_b.start()
    gathers[0].settle()
    scatter_at(1).settle()
    ex_b.add()
    ex_a.finish()
    save_dattn.wait(0)
    ex_b.finish()
    for l in range(n_layers):
        for i in range(6):
            if l == 0 and i < 2:
                val = r.sum_b[i:i + 1]
            else:
                at = i - 2 if l == 0 else 6 * l - 2 + i
                val = r.sum_a[at:at + 1]
            if i < 4:
                r.ln_grad[l, i:i + 1] = val
            else:
                r.bias_grad[l, i - 4:i - 3] = val


def solution(mesh):
    n = mesh.shape['tp']

    def device_step(x_loc, dy_loc, ln_par, bias_d, w_qkv, w_out, w_up, b_up, w_down):
        n_layers = ln_par.shape[0]
        rows, width = x_loc.shape[1:]
        e, f = w_qkv.shape[-1], w_up.shape[-1]
        nz = n // 2
        far = nz // 2
        size = rows // PIECES
        steps = PIECES * (far - 1) + PIECES // 2
        blk = (nz, 2 * rows)
        seq = n * rows
        few = 8 * (-(-(6 * n_layers - 2) // 8))
        cols = width // n
        hbm = dict(
            h_one=(blk + (width,), BF16), h_two=(blk + (width,), BF16), pre_h=(blk + (f,), F32), act_h=(blk + (f,), BF16),
            prob_h=(blk + (seq,), BF16), q_h=(blk + (e,), BF16), k_h=(blk + (e,), BF16), v_h=(blk + (e,), BF16),
            attn_h=(blk + (e,), BF16))
        saved = {name: ((n_layers,) + shape, dtype, ANY) for name, (shape, dtype) in hbm.items()}
        saved['dy_all'] = (blk + (width,), BF16, ANY)
        saved['res'] = ((2 * n_layers, rows, width), F32, VM)
        dma = pltpu.SemaphoreType.DMA

        def comm(lands, signals):
            return dict(
                all=pltpu.VMEM((3,) + blk + (width,), BF16), own=pltpu.VMEM((2, rows, width), BF16),
                part=pltpu.VMEM((HELD, 2 * rows, width), F32), give=pltpu.VMEM((nz, rows, width), BF16),
                pair=pltpu.VMEM((2, nz, rows, width), BF16), send=pltpu.VMEM((2, steps, size, width), BF16),
                recv=pltpu.VMEM((2, 2, steps, size, width), BF16),
                wq_v=pltpu.VMEM((width, 3 * e), BF16), wo_v=pltpu.VMEM((e, width), BF16),
                wu_v=pltpu.VMEM((width, f), BF16), wd_v=pltpu.VMEM((f, width), BF16),
                q=pltpu.VMEM((n_layers,) + blk + (e,), BF16), k=pltpu.VMEM((n_layers,) + blk + (e,), BF16),
                v=pltpu.VMEM((n_layers,) + blk + (e,), BF16), attn=pltpu.VMEM((n_layers,) + blk + (e,), BF16),
                prob=pltpu.VMEM(blk + (seq,), BF16), pre=pltpu.VMEM(blk + (f,), F32),
                act=pltpu.VMEM((n_layers,) + blk + (f,), BF16),
                gs=dma((lands, 4, 2, far + 1, PIECES)), ss=dma((2, 2, 2, steps)), ps=dma((2, 2, nz)), local=dma((signals,)))

        def call(body, cid, inputs, outputs, scratch):
            names = list(inputs) + list(outputs) + list(scratch)

            def kernel(*refs):
                body(types.SimpleNamespace(**dict(zip(names, refs))), n, n_layers)

            out = pl.pallas_call(
                kernel, out_shape=[jax.ShapeDtypeStruct(shape, dtype) for shape, dtype, _ in outputs.values()],
                in_specs=[spec for _, spec in inputs.values()], out_specs=[spec for _, _, spec in outputs.values()],
                scratch_shapes=list(scratch.values()),
                compiler_params=pltpu.CompilerParams(collective_id=cid, has_side_effects=True, vmem_limit_bytes=67043328),
                name=body.__name__)(*[arr for arr, _ in inputs.values()])
            return types.SimpleNamespace(**dict(zip(outputs, out)))

        weights = dict(
            dy=(dy_loc[0], VM), ln=(ln_par, VM), wq=(jnp.transpose(w_qkv[:, :, :, 0], (0, 2, 1, 3)), ANY),
            wo=(w_out[:, 0], ANY), wu=(w_up, ANY), wd=(w_down, ANY))
        fwd = call(
            forward_kernel, 1, dict(x=(x_loc[0], VM), bias=(bias_d, VM), bup=(b_up[:, None], VM), **weights),
            dict(y=((rows, width), BF16, VM), **saved), comm(3, 24))
        bwd = call(
            backward_kernel, 2, dict(weights, **{name: (getattr(fwd, name), spec) for name, (_, _, spec) in saved.items()}),
            dict(
                dx=((rows, width), BF16, VM), ln_grad=(ln_par.shape, F32, VM), bias_grad=(bias_d.shape, F32, VM),
                dwq=((n_layers, 3, width, e), BF16, ANY), dwo=((n_layers, e, width), BF16, ANY),
                dwu=(w_up.shape, BF16, ANY), d_bup=(b_up.shape, F32, VM), dwd=(w_down.shape, BF16, ANY)),
            dict(
                comm(2, 32), d_res=pltpu.VMEM((rows, width), F32), d_pre=pltpu.VMEM(blk + (f,), BF16),
                d_proj=pltpu.VMEM(blk + (3 * e,), BF16), d_k=pltpu.VMEM((seq, e), F32), d_v=pltpu.VMEM((seq, e), F32),
                bup_sum=pltpu.VMEM((1, f), F32), dwq_v=pltpu.VMEM((3, width, e), BF16), dwo_v=pltpu.VMEM((e, width), BF16),
                dwu_v=pltpu.VMEM((width, f), BF16), dwd_v=pltpu.VMEM((f, width), BF16),
                small_a=pltpu.VMEM((few, width), F32), small_b=pltpu.VMEM((8, width), F32),
                got_a=pltpu.VMEM((n, few, cols), F32), got_b=pltpu.VMEM((n, 8, cols), F32),
                sum_a=pltpu.VMEM((few, width), F32), sum_b=pltpu.VMEM((8, width), F32), es=dma((2, 4, n))))
        return (fwd.y[None], bwd.dx[None], bwd.ln_grad, bwd.bias_grad, jnp.transpose(bwd.dwq, (0, 2, 1, 3))[:, :, :, None],
                bwd.dwo[:, None], bwd.dwu, bwd.d_bup, bwd.dwd)

    in_specs = (P('dp', 'tp', None), P('dp', 'tp', None), P(None, None, None), P(None, None, None),
                P(None, None, None, 'tp', None), P(None, 'tp', None, None), P(None, None, 'tp'), P(None, 'tp'), P(None, 'tp', None))
    out_specs = (P('dp', 'tp', None), P('dp', 'tp', None), P('dp', None, None), P('dp', None, None),
                 P('dp', None, None, 'tp', None), P('dp', 'tp', None, None), P('dp', None, 'tp'), P('dp', 'tp'), P('dp', 'tp', None))
    return jax.shard_map(device_step, mesh=mesh, in_specs=in_specs, out_specs=out_specs, check_vma=False)
```

```python
import math
import types

import jax
import jax.numpy as jnp
from jax import lax
from jax.experimental import pallas as pl
from jax.experimental.pallas import tpu as pltpu
from jax.sharding import PartitionSpec as P

F32 = jnp.float32
BF16 = jnp.bfloat16
MESH = pl.DeviceIdType.MESH
VM = pl.BlockSpec(memory_space=pltpu.VMEM)
ANY = pl.BlockSpec(memory_space=pl.ANY)
PIECES = 4
HELD = 5
TILE = 256
FINAL = (2, 0, 3, 1)
GATHER = {1: ((2, 0, 3, 1), (2, 0, 3, 1)), -1: ((2, 0, 3, 1), (2, 3, 0, 1), (3, 2, 1, 0))}
GATHER_FAR = {1: (2, 0), -1: (3, 1)}
SCATTER_FAR = {1: (0, 1), -1: (2, 3)}
SCATTER = {1: (2, 3, 0, 1), -1: (0, 1, 2, 3)}
SCATTER_TWO = {1: (2, 3, 0, 1), -1: (0, 2, 1, 3)}


def side(d):
    return (1 - d) // 2


def remote(src, dst, send_sem, recv_sem, dev):
    return pltpu.make_async_remote_copy(src_ref=src, dst_ref=dst, send_sem=send_sem, recv_sem=recv_sem,
                                        device_id={'tp': dev}, device_id_type=MESH)


class Ring:
    def __init__(self, n):
        self.n = n
        self.nz = n // 2
        self.far = self.nz // 2
        self.me = lax.axis_index('tp')
        self.z = self.me // 2
        self.c = lax.rem(self.me, 2)
        self.sib = self.me + 1 - 2 * self.c
        self.next = {1: lax.rem(self.me + 2, n), -1: lax.rem(self.me + n - 2, n)}
        self.peers = [lax.rem(self.me + j, n) for j in range(n)]

    def chip(self, off):
        return lax.rem(self.z + (off + self.nz), self.nz)

    def enter(self, devices):
        bar = pltpu.get_barrier_semaphore()
        for dev in devices:
            pl.semaphore_signal(bar, inc=1, device_id={'tp': dev}, device_id_type=MESH)
        pl.semaphore_wait(bar, len(devices))


class Gather:
    def __init__(self, ring, own, land, sems):
        self.ring, self.own, self.land = ring, own, land
        self.sems = sems
        self.rows = own.shape[0]
        self.size = self.rows // PIECES

    def piece(self, off, core, q):
        return self.land.at[self.ring.chip(off), pl.ds(pl.multiple_of(core * self.rows + q * self.size, self.size), self.size)]

    def order(self, d, k):
        if k == self.ring.far - 1:
            return GATHER_FAR[d]
        return GATHER[d][min(k, len(GATHER[d]) - 1)]

    def forward(self, d, k, q):
        dst = self.piece(-d * k, self.ring.c, q)
        src = self.own.at[pl.ds(q * self.size, self.size)] if k == 0 else dst
        return remote(src, dst, self.sems[0].at[side(d), k, q], self.sems[1].at[side(d), k, q], self.ring.next[d])

    def arrival(self, d, k, q):
        ref = self.piece(-d * (k + 1), self.ring.c, q)
        return remote(ref, ref, self.sems[0].at[side(d), k, q], self.sems[1].at[side(d), k, q], self.ring.next[d])

    def pair(self, d, k, q, core):
        ref = self.piece(-d * (k + 1), core, q)
        return remote(ref, ref, self.sems[2].at[side(d), k, q], self.sems[3].at[side(d), k, q], self.ring.sib)

    def own_pair(self, q, core):
        far = self.ring.far
        return remote(self.own.at[pl.ds(q * self.size, self.size)], self.piece(0, core, q),
                      self.sems[2].at[0, far, q], self.sems[3].at[0, far, q], self.ring.sib)

    def launch(self, q):
        for d in (1, -1):
            self.forward(d, 0, q).start()
        self.own_pair(q, self.ring.c).start()

    def place_own(self):
        self.land[self.ring.z, pl.ds(pl.multiple_of(self.ring.c * self.rows, self.rows), self.rows)] = self.own[...]
        for q in range(PIECES):
            self.own_pair(q, 1 - self.ring.c).wait_recv()

    def hop(self, k):
        far = self.ring.far
        wait = {d: list(self.order(d, k + 1)) if k + 1 < far else [] for d in (1, -1)}
        have = {1: set(), -1: set()}
        for i in range(len(self.order(1, k))):
            for d in (1, -1):
                q = self.order(d, k)[i]
                self.arrival(d, k, q).wait_recv()
                have[d].add(q)
                while wait[d] and wait[d][0] in have[d]:
                    self.forward(d, k + 1, wait[d].pop(0)).start()
                self.pair(d, k, q, self.ring.c).start()

    def paired(self, k):
        for d in (1, -1):
            for q in self.order(d, k):
                self.pair(d, k, q, 1 - self.ring.c).wait_recv()

    def offs(self, k):
        return (k + 1, -(k + 1)) if k < self.ring.far - 1 else (self.ring.far,)

    def run(self, on_hop, middle):
        self.place_own()
        on_hop([self.ring.z], True)
        for k in range(self.ring.far):
            self.hop(k)
            if k == self.ring.far - 2:
                middle()
            self.paired(k)
            on_hop([self.ring.chip(o) for o in self.offs(k)], False)

    def settle(self):
        for d in (1, -1):
            for k in range(self.ring.far):
                for q in self.order(d, k):
                    self.forward(d, k, q).wait_send()
                    self.pair(d, k, q, self.ring.c).wait_send()
        for q in range(PIECES):
            self.own_pair(q, self.ring.c).wait_send()


class Scatter:
    def __init__(self, ring, part, give, pair, send, recv, sems):
        self.ring, self.part, self.give, self.pair_ref, self.send, self.recv = ring, part, give, pair, send, recv
        self.sems = sems
        self.rows = give.shape[1]
        self.size = self.rows // PIECES
        far = ring.far
        self.offs = [far]
        for k in range(far - 1, 0, -1):
            self.offs += [k, -k]
        self.offs.append(0)
        self.slots = {}
        for d in (1, -1):
            self.slots[d] = [(far, q) for q in SCATTER_FAR[d]]
            for k in range(far - 1, 0, -1):
                order = FINAL if k == 1 else SCATTER_TWO[d] if k == 2 else SCATTER[d]
                self.slots[d] += [(k, q) for q in order]
        self.steps = len(self.slots[1])
        self.paired = set()
        self.made = 0

    def pair(self, j):
        return remote(self.give.at[j], self.pair_ref.at[j], self.sems[2].at[j], self.sems[3].at[j], self.ring.sib)

    def hop(self, d, s):
        i = side(d)
        return remote(self.send.at[i, s], self.recv.at[i, s], self.sems[0].at[i, s], self.sems[1].at[i, s], self.ring.next[d])

    def fill(self, make):
        j = self.made
        self.part[j % HELD] = make(self.offs[j])
        theirs = pl.ds(pl.multiple_of((1 - self.ring.c) * self.rows, self.rows), self.rows)
        self.give[j] = self.part[j % HELD, theirs].astype(BF16)
        self.pair(j).start()
        self.made += 1

    def base(self, j, q):
        if j not in self.paired:
            self.pair(j).wait_recv()
            self.paired.add(j)
        at = pl.multiple_of(self.ring.c * self.rows + q * self.size, self.size)
        return self.part[j % HELD, pl.ds(at, self.size)] + self.pair_ref[j, pl.ds(q * self.size, self.size)].astype(F32)

    def run(self, make, work=None, count=0):
        n_off = len(self.offs)
        fill_after = {0: 2}
        for j in range(3, n_off):
            fill_after[min(2 * (j - 2), self.steps - PIECES - (n_off - 1 - j) - 1)] = j
        quiet = [s for s in range(3, self.steps - 1, 4) if s not in fill_after] + [self.steps - 2]
        begun = 0
        self.fill(make)
        self.fill(make)
        for s in range(self.steps):
            for d in (1, -1):
                k, q = self.slots[d][s]
                val = self.base(self.offs.index(d * k if k < self.ring.far else self.ring.far), q)
                if (k + 1, q) in self.slots[d]:
                    t = self.slots[d].index((k + 1, q))
                    self.hop(d, t).wait_recv()
                    val = val + self.recv[side(d), t].astype(F32)
                self.send[side(d), s] = val.astype(BF16)
                self.hop(d, s).start()
            if s in fill_after:
                self.fill(make)
            elif s in quiet and begun < count:
                upto = begun + -(-(count - begun) // len([t for t in quiet if t >= s]))
                if upto - begun == 1:
                    work(begun)
                else:
                    pl.loop(begun, upto)(work)
                begun = upto

    def total(self, q):
        val = self.base(len(self.offs) - 1, q)
        for d in (1, -1):
            s = self.slots[d].index((1, q))
            self.hop(d, s).wait_recv()
            val = val + self.recv[side(d), s].astype(F32)
        return val

    def settle(self):
        for d in (1, -1):
            for s in range(self.steps):
                self.hop(d, s).wait_send()
        for j in range(len(self.offs)):
            self.pair(j).wait_send()


class Exchange:
    def __init__(self, ring, rows, got, out, sems):
        self.ring, self.rows, self.got, self.out = ring, rows, got, out
        self.sems = sems
        self.cols = rows.shape[1] // ring.n

    def block(self, ref, dev):
        return ref.at[:, pl.ds(pl.multiple_of(dev * self.cols, self.cols), self.cols)]

    def first(self, j):
        peer = self.ring.peers[j]
        return remote(self.block(self.rows, peer), self.got.at[j], self.sems[0].at[j], self.sems[1].at[j], peer)

    def second(self, j, dev):
        return remote(self.got.at[0], self.block(self.out, dev), self.sems[2].at[j], self.sems[3].at[j], self.ring.peers[j])

    def start(self):
        for j in range(1, self.ring.n):
            self.first(j).start()

    def add(self):
        mine = pl.ds(pl.multiple_of(self.ring.me * self.cols, self.cols), self.cols)
        acc = self.rows[:, mine]
        for j in range(1, self.ring.n):
            self.first(j).wait_recv()
            acc = acc + self.got[j]
        self.got[0] = acc
        self.out[:, mine] = acc
        for j in range(1, self.ring.n):
            self.second(j, self.ring.me).start()

    def finish(self):
        for j in range(1, self.ring.n):
            self.second(j, lax.rem(self.ring.me + self.ring.n - j, self.ring.n)).wait_recv()
        for j in range(1, self.ring.n):
            self.first(j).wait_send()
            self.second(j, self.ring.me).wait_send()


class Local:
    def __init__(self, sems):
        self.sems = sems
        self.used = 0

    def copies(self, *pairs):
        at = self.used
        self.used += len(pairs)

        def of(l):
            return [pltpu.make_async_copy(*pair(l), self.sems.at[at + i]) for i, pair in enumerate(pairs)]

        return types.SimpleNamespace(start=lambda l: [c.start() for c in of(l)], wait=lambda l: [c.wait() for c in of(l)])


def dot(a, b, ca=1, cb=0):
    return lax.dot_general(a, b, (((ca,), (cb,)), ((), ())), preferred_element_type=F32)


def layer_norm(row_vals, ln_gain, ln_shift):
    mean_val = jnp.mean(row_vals, axis=-1, keepdims=True)
    centered = row_vals - mean_val
    var_val = jnp.mean(centered * centered, axis=-1, keepdims=True)
    return centered * lax.rsqrt(var_val + 1e-5) * ln_gain + ln_shift


def layer_norm_back(d_out, row_vals, ln_gain):
    mean_val = jnp.mean(row_vals, axis=-1, keepdims=True)
    centered = row_vals - mean_val
    var_val = jnp.mean(centered * centered, axis=-1, keepdims=True)
    inv = lax.rsqrt(var_val + 1e-5)
    unit = centered * inv
    scaled = d_out * ln_gain
    pull = scaled - jnp.mean(scaled, axis=-1, keepdims=True) - unit * jnp.mean(scaled * unit, axis=-1, keepdims=True)
    return pull * inv, d_out * unit


GELU_C = math.sqrt(2.0 / math.pi)


def gelu(x):
    return x * (0.5 * (1.0 + jnp.tanh(GELU_C * (x + 0.044715 * (x * x * x)))))


def gelu_slope(x):
    t = jnp.tanh(GELU_C * (x + 0.044715 * (x * x * x)))
    return 0.5 * (1.0 + t) + 0.5 * x * (1.0 - t * t) * (GELU_C * (1.0 + 3 * 0.044715 * (x * x)))


def rows_of(ref, chips):
    parts = [ref[z] for z in chips]
    return parts[0] if len(parts) == 1 else jnp.concatenate(parts, axis=0)


def put_rows(ref, chips, vals):
    m = ref.shape[1]
    for i, z in enumerate(chips):
        ref[z] = vals[i * m:(i + 1) * m].astype(ref.dtype)


def flat(ref, cols=None):
    vals = ref[...] if cols is None else ref[:, :, cols]
    return vals.reshape(vals.shape[0] * vals.shape[1], vals.shape[2])


def col_sum(vals):
    return jnp.sum(vals, axis=0, keepdims=True)


def forward_kernel(r, n, n_layers):
    ring = Ring(n)
    local = Local(r.local)
    rows, width = r.dy.shape
    e = r.wq.shape[-1]
    size = rows // PIECES
    scale = e ** -0.5
    last = n_layers - 1
    gathers = [Gather(ring, own, r.all.at[i], [r.gs.at[i, t] for t in range(4)])
               for i, own in enumerate((r.own.at[0], r.own.at[1], r.dy))]

    def scatter_at(i):
        return Scatter(ring, r.part, r.give, r.pair.at[i], r.send, r.recv.at[i],
                       [r.ss.at[i, 0], r.ss.at[i, 1], r.ps.at[i, 0], r.ps.at[i, 1]])

    def piece(q):
        return pl.ds(q * size, size)

    attn_w = local.copies(*[lambda l, i=i: (r.wq.at[l, i], r.wq_v.at[:, pl.ds(i * e, e)]) for i in range(3)],
                          lambda l: (r.wo.at[l], r.wo_v))
    mlp_w = local.copies(lambda l: (r.wd.at[l], r.wd_v), lambda l: (r.wu.at[l], r.wu_v))
    dy = gathers[2]
    save_one = local.copies(lambda l: (r.all.at[0], r.h_one.at[l]), *[lambda l, a=a, b=b: (a.at[l], b.at[l]) for a, b in
                                                                      ((r.q, r.q_h), (r.k, r.k_h), (r.v, r.v_h))])
    save_attn = local.copies(lambda l: (r.prob, r.prob_h.at[l]), lambda l: (r.attn.at[l], r.attn_h.at[l]),
                             lambda l: (r.wqt_v, r.wqt.at[l]), lambda l: (r.wot_v, r.wot.at[l]))
    save_turn = local.copies(lambda l: (r.wut_v, r.wut.at[l]), lambda l: (r.wdt_v, r.wdt.at[l]))
    save_mlp = local.copies(lambda l: (r.all.at[1], r.h_two.at[l]), lambda l: (r.pre, r.pre_h.at[l]),
                            lambda l: (r.act.at[l], r.act_h.at[l]))
    save_dy = local.copies(lambda l: (r.all.at[2], r.dy_all))

    attn_w.start(0)
    mlp_w.start(0)
    for q in FINAL:
        res = r.x[piece(q)].astype(F32)
        r.res[0, piece(q)] = res
        r.own[0, piece(q)] = layer_norm(res, r.ln[0, 0:1], r.ln[0, 1:2]).astype(BF16)
    ring.enter([ring.next[1], ring.next[-1], ring.sib])
    for q in FINAL:
        gathers[0].launch(q)

    def side_steps(phase, odd):
        for k in range(odd, min(2 * n_layers, ring.far), 2):
            @pl.when(phase == k)
            def _():
                if k == 0:
                    for q in FINAL:
                        dy.launch(q)
                else:
                    dy.hop(k - 1)

    @pl.loop(0, n_layers)
    def forward(l):
        inner = l < last

        def on_attn(chips, first):
            if first:
                attn_w.wait(l)
            vals = dot(rows_of(r.all.at[0], chips), r.wq_v[...]).astype(BF16)
            for i, ref in enumerate((r.q, r.k, r.v)):
                put_rows(ref.at[l], chips, vals[:, i * e:(i + 1) * e])

        def middle():
            side_steps(2 * l, 0)

            @pl.when(l > 0)
            def _():
                gathers[1].settle()
                scatter_at(1).settle()
                save_mlp.wait(l)
                save_turn.wait(l)

        gathers[0].run(on_attn, middle)
        save_one.start(l)

        def turn_attn(j):
            at = pl.ds(pl.multiple_of(j * TILE, TILE), TILE)
            r.wqt_v[:, at] = r.wq_v[at].T
            r.wot_v[at] = r.wo_v[:, at].T

        def make(off):
            chip = ring.chip(off)
            s = dot(r.q[l, chip], flat(r.k.at[l]), 1, 1) * scale
            row = lax.broadcasted_iota(jnp.int32, s.shape, 0) + chip * (2 * rows)
            col = lax.broadcasted_iota(jnp.int32, s.shape, 1)
            s = jnp.where(row >= col, s, -1e30)
            s = jnp.exp(s - jnp.max(s, axis=-1, keepdims=True))
            p = (s / jnp.sum(s, axis=-1, keepdims=True)).astype(BF16)
            r.prob[chip] = p
            a = dot(p, flat(r.v.at[l])).astype(BF16)
            r.attn[l, chip] = a
            return dot(a, r.wo_v[...])

        sc = scatter_at(0)
        sc.run(make, turn_attn, width // TILE)
        for q in FINAL:
            res = r.res[2 * l, piece(q)] + sc.total(q) + r.bias[l, 0:1]
            r.res[2 * l + 1, piece(q)] = res
            r.own[1, piece(q)] = layer_norm(res, r.ln[l, 2:3], r.ln[l, 3:4]).astype(BF16)
            gathers[1].launch(q)
        save_attn.start(l)

        @pl.when(inner)
        def _():
            attn_w.start(l + 1)

        def on_mlp(chips, first):
            if first:
                mlp_w.wait(l)
            pre = dot(rows_of(r.all.at[1], chips), r.wu_v[...]) + r.bup[l]
            put_rows(r.pre, chips, pre)
            put_rows(r.act.at[l], chips, gelu(pre))

        def middle_two():
            side_steps(2 * l + 1, 1)
            gathers[0].settle()
            scatter_at(0).settle()
            save_one.wait(l)
            save_attn.wait(l)

        gathers[1].run(on_mlp, middle_two)
        save_mlp.start(l)

        def turn_mlp(j):
            at = pl.ds(pl.multiple_of(j * TILE, TILE), TILE)
            r.wut_v[:, at] = r.wu_v[at].T
            r.wdt_v[at] = r.wd_v[:, at].T

        sc = scatter_at(1)
        sc.run(lambda off: dot(r.act[l, ring.chip(off)], r.wd_v[...]), turn_mlp, width // TILE)
        save_turn.start(l)
        for q in FINAL:
            res = r.res[2 * l + 1, piece(q)] + sc.total(q) + r.bias[l, 1:2]
            r.y[piece(q)] = res.astype(BF16)

            @pl.when(inner)
            def _():
                r.res[2 * l + 2, piece(q)] = res
                r.own[0, piece(q)] = layer_norm(res, r.ln[l + 1, 0:1], r.ln[l + 1, 1:2]).astype(BF16)
                gathers[0].launch(q)

        @pl.when(inner)
        def _():
            mlp_w.start(l + 1)

    for k in range(min(2 * n_layers, ring.far) - 1, ring.far):
        dy.hop(k)
    dy.place_own()
    for k in range(ring.far):
        dy.paired(k)

    save_dy.start(0)
    dy.settle()
    gathers[1].settle()
    scatter_at(1).settle()
    save_mlp.wait(last)
    save_turn.wait(last)
    save_dy.wait(0)


def backward_kernel(r, n, n_layers):
    ring = Ring(n)
    local = Local(r.local)
    rows, width = r.dy.shape
    e = r.q.shape[-1]
    size = rows // PIECES
    scale = e ** -0.5
    last = n_layers - 1
    gathers = [Gather(ring, own, r.all.at[i], [r.gs.at[i, t] for t in range(4)])
               for i, own in enumerate((r.own.at[0], r.own.at[1]))]

    def scatter_at(i):
        return Scatter(ring, r.part, r.give, r.pair.at[i], r.send, r.recv.at[i],
                       [r.ss.at[i, 0], r.ss.at[i, 1], r.ps.at[i, 0], r.ps.at[i, 1]])

    def piece(q):
        return pl.ds(q * size, size)

    attn_w = local.copies(lambda l: (r.wot.at[l], r.wot_v), lambda l: (r.wqt.at[l], r.wqt_v))
    mlp_w = local.copies(lambda l: (r.wdt.at[l], r.wdt_v), lambda l: (r.wut.at[l], r.wut_v))
    blocks = width // TILE
    load_one = local.copies(lambda l: (r.h_one.at[l], r.all.at[2]))
    load_two = local.copies(lambda l: (r.h_two.at[l], r.all.at[2]))
    load_top = local.copies(lambda l: (r.dy_all, r.all.at[2]))
    load_top_two = local.copies(lambda l: (r.h_two.at[l], r.all.at[1]))
    load_prob = local.copies(lambda l: (r.prob_h.at[l], r.prob))
    load_pre = local.copies(lambda l: (r.pre_h.at[l], r.pre))
    load_act = local.copies(lambda l: (r.act_h, r.act))
    load_attn = local.copies(*[lambda l, a=a, b=b: (a, b) for a, b in
                               ((r.q_h, r.q), (r.k_h, r.k), (r.v_h, r.v), (r.attn_h, r.attn))])
    save_dmlp = local.copies(lambda l: (r.dwd_v, r.dwd.at[l]), lambda l: (r.dwu_v, r.dwu.at[l]))
    save_dattn = local.copies(lambda l: (r.dwo_v, r.dwo.at[l]), lambda l: (r.dwq_v, r.dwq.at[l]))

    load_top.start(0)
    load_pre.start(last)
    mlp_w.start(last)
    load_top_two.start(last)
    load_act.start(0)
    attn_w.start(last)
    load_prob.start(last)
    load_attn.start(0)
    for q in FINAL:
        r.d_res[piece(q)] = r.dy[piece(q)].astype(F32)
    r.small_a[...] = jnp.zeros_like(r.small_a)
    r.small_b[...] = jnp.zeros_like(r.small_b)
    ring.enter(ring.peers[1:])

    def put_small(l, i, val):
        for m in range(n_layers):
            @pl.when(l == m)
            def _():
                if m == 0 and i < 2:
                    r.small_b[i:i + 1] = val
                else:
                    at = i - 2 if m == 0 else 6 * m - 2 + i
                    r.small_a[at:at + 1] = val

    def backward_tail(sc, res_at, gain, after, out):
        d_gain = d_shift = d_bias = 0.0
        for q in FINAL:
            d_h = sc.total(q)
            d_in, terms = layer_norm_back(d_h, r.res[res_at, piece(q)], gain)
            d_new = r.d_res[piece(q)] + d_in
            out(q, d_new)
            d_gain, d_shift, d_bias = d_gain + col_sum(terms), d_shift + col_sum(d_h), d_bias + col_sum(d_new)
            r.d_res[piece(q)] = d_new
        after(d_gain, d_shift, d_bias)

    put_small(last, 5, col_sum(r.d_res[...]))
    ex_a = Exchange(ring, r.small_a, r.got_a, r.sum_a, [r.es.at[0, t] for t in range(4)])
    ex_b = Exchange(ring, r.small_b, r.got_b, r.sum_b, [r.es.at[1, t] for t in range(4)])

    @pl.loop(0, n_layers)
    def backward(i):
        l = last - i
        top, lower = i == 0, i > 0
        at_d = 1 + (n_layers - i) // n_layers
        at_h = 3 - at_d

        @pl.when(lower)
        def _():
            load_two.start(l)
            load_prob.start(l)

        r.bup_sum[...] = jnp.zeros_like(r.bup_sum)

        def on_mlp(chips, first):
            if first:
                mlp_w.wait(l)
                load_pre.wait(l)
            d_act = dot(rows_of(r.all.at[at_d], chips), r.wdt_v[...])
            d_pre = d_act * gelu_slope(rows_of(r.pre, chips))
            r.bup_sum[...] += col_sum(d_pre)
            put_rows(r.d_pre, chips, d_pre)

        @pl.when(lower)
        def _():
            def middle():
                gathers[0].settle()
                scatter_at(1).settle()
                save_dattn.wait(l)
                load_two.wait(l)

            gathers[1].run(on_mlp, middle)

        @pl.when(top)
        def _():
            load_top.wait(0)
            load_pre.wait(l)
            mlp_w.wait(l)

            @pl.loop(0, ring.far)
            def _(z):
                on_mlp([z, z + ring.far], False)

            load_top_two.wait(l)
            load_act.wait(0)

        def mlp_work(j):
            cols = pl.ds(pl.multiple_of(j * TILE, TILE), TILE)
            r.dwd_v[:, cols] = dot(flat(r.act.at[l]), flat(r.all.at[at_d], cols), 0, 0).astype(BF16)
            r.dwu_v[cols] = dot(flat(r.all.at[at_h], cols), flat(r.d_pre), 0, 0).astype(BF16)

        sc = scatter_at(0)
        sc.run(lambda off: dot(r.d_pre[ring.chip(off)], r.wut_v[...]), mlp_work, blocks)
        save_dmlp.start(l)

        def hand_on(q, d_new):
            r.own[0, piece(q)] = d_new.astype(BF16)
            gathers[0].launch(q)

        def after_mlp(d_gain, d_shift, d_bias):
            put_small(l, 2, d_gain)
            put_small(l, 3, d_shift)
            put_small(l, 4, d_bias)
            for m in range(n_layers):
                @pl.when(l == m)
                def _():
                    r.d_bup[m:m + 1] = r.bup_sum[...]

        backward_tail(sc, 2 * l + 1, r.ln[l, 2:3], after_mlp, hand_on)

        @pl.when(l > 0)
        def _():
            load_pre.start(l - 1)
            mlp_w.start(l - 1)

        @pl.when(l == 0)
        def _():
            ex_a.start()

        load_one.start(l)
        r.d_k[...] = jnp.zeros_like(r.d_k)
        r.d_v[...] = jnp.zeros_like(r.d_v)

        def on_attn(chips, first):
            if first:
                attn_w.wait(l)
                load_prob.wait(l)

                @pl.when(top)
                def _():
                    load_attn.wait(0)
            d_attn = dot(rows_of(r.all.at[0], chips), r.wot_v[...]).astype(BF16)
            prob = rows_of(r.prob, chips)
            d_prob = dot(d_attn, flat(r.v.at[l]), 1, 1)
            row_dot = jnp.sum(d_prob * prob, axis=-1, keepdims=True)
            d_score = (prob * (d_prob - row_dot) * scale).astype(BF16)
            d_q = dot(d_score, flat(r.k.at[l])).astype(BF16)
            for t, z in enumerate(chips):
                r.d_proj[z, :, 0:e] = d_q[t * 2 * rows:(t + 1) * 2 * rows]
            r.d_k[...] += dot(d_score, rows_of(r.q.at[l], chips), 0, 0)
            r.d_v[...] += dot(prob, d_attn, 0, 0)

        def middle_two():
            @pl.when(lower)
            def _():
                gathers[1].settle()

            scatter_at(0).settle()
            save_dmlp.wait(l)
            load_one.wait(l)

        gathers[0].run(on_attn, middle_two)
        blk = r.d_proj.shape[:2] + (e,)
        r.d_proj[:, :, e:2 * e] = r.d_k[...].astype(BF16).reshape(blk)
        r.d_proj[:, :, 2 * e:] = r.d_v[...].astype(BF16).reshape(blk)

        def attn_work(j):
            cols = pl.ds(pl.multiple_of(j * TILE, TILE), TILE)
            r.dwo_v[:, cols] = dot(flat(r.attn.at[l]), flat(r.all.at[0], cols), 0, 0).astype(BF16)
            vals = dot(flat(r.all.at[2], cols), flat(r.d_proj), 0, 0).astype(BF16)
            for t in range(3):
                r.dwq_v[t, cols] = vals[:, t * e:(t + 1) * e]

        sc = scatter_at(1)
        sc.run(lambda off: dot(r.d_proj[ring.chip(off)], r.wqt_v[...]), attn_work, blocks)
        save_dattn.start(l)

        @pl.when(l == 0)
        def _():
            ex_a.add()

        def out(q, d_new):
            r.dx[piece(q)] = d_new.astype(BF16)

            @pl.when(l > 0)
            def _():
                r.own[1, piece(q)] = d_new.astype(BF16)
                gathers[1].launch(q)

        def after_attn(d_gain, d_shift, d_bias):
            put_small(l, 0, d_gain)
            put_small(l, 1, d_shift)
            put_small(l - 1, 5, d_bias)

        backward_tail(sc, 2 * l, r.ln[l, 0:1], after_attn, out)

        @pl.when(l > 0)
        def _():
            attn_w.start(l - 1)

    ex_b.start()
    gathers[0].settle()
    scatter_at(1).settle()
    ex_b.add()
    ex_a.finish()
    save_dattn.wait(0)
    ex_b.finish()
    for l in range(n_layers):
        for i in range(6):
            if l == 0 and i < 2:
                val = r.sum_b[i:i + 1]
            else:
                at = i - 2 if l == 0 else 6 * l - 2 + i
                val = r.sum_a[at:at + 1]
            if i < 4:
                r.ln_grad[l, i:i + 1] = val
            else:
                r.bias_grad[l, i - 4:i - 3] = val


def write_out(*results):
    parts = [(a, i) for a in sorted(range(len(results)), key=lambda a: -results[a].size)
             for i in (range(results[a].shape[0]) if results[a].ndim > 2 else [None])]

    def body(*refs):
        m = len(results)
        ins, outs, bufs, sems = refs[:m], refs[m:2 * m], refs[2 * m:3 * m], refs[3 * m]

        def at(ref, i):
            return ref if i is None else ref.at[i]

        reads = [pltpu.make_async_copy(at(ins[a], i), at(bufs[a], i), sems.at[0, t]) for t, (a, i) in enumerate(parts)]
        writes = [pltpu.make_async_copy(at(bufs[a], i), at(outs[a], i), sems.at[1, t]) for t, (a, i) in enumerate(parts)]
        for copy in reads:
            copy.start()
        for read, write in zip(reads, writes):
            read.wait()
            write.start()
        for write in writes:
            write.wait()

    return pl.pallas_call(
        body, out_shape=[jax.ShapeDtypeStruct(a.shape, a.dtype) for a in results], in_specs=[ANY] * len(results),
        out_specs=[ANY] * len(results),
        scratch_shapes=[pltpu.VMEM(a.shape, a.dtype) for a in results] + [pltpu.SemaphoreType.DMA((2, len(parts)))],
        compiler_params=pltpu.CompilerParams(vmem_limit_bytes=67043328), name='write_out')(*results)


def solution(mesh):
    n = mesh.shape['tp']

    def device_step(x_loc, dy_loc, ln_par, bias_d, w_qkv, w_out, w_up, b_up, w_down):
        n_layers = ln_par.shape[0]
        rows, width = x_loc.shape[1:]
        e, f = w_qkv.shape[-1], w_up.shape[-1]
        nz = n // 2
        far = nz // 2
        size = rows // PIECES
        steps = PIECES * (far - 1) + PIECES // 2
        blk = (nz, 2 * rows)
        seq = n * rows
        few = 8 * (-(-(6 * n_layers - 2) // 8))
        cols = width // n
        hbm = dict(
            h_one=(blk + (width,), BF16), h_two=(blk + (width,), BF16), pre_h=(blk + (f,), F32), act_h=(blk + (f,), BF16),
            prob_h=(blk + (seq,), BF16), q_h=(blk + (e,), BF16), k_h=(blk + (e,), BF16), v_h=(blk + (e,), BF16),
            attn_h=(blk + (e,), BF16),
            wqt=((3 * e, width), BF16), wot=((width, e), BF16), wut=((f, width), BF16), wdt=((width, f), BF16))
        saved = {name: ((n_layers,) + shape, dtype, ANY) for name, (shape, dtype) in hbm.items()}
        saved['dy_all'] = (blk + (width,), BF16, ANY)
        saved['res'] = ((2 * n_layers, rows, width), F32, VM)
        dma = pltpu.SemaphoreType.DMA

        def comm(lands, signals):
            return dict(
                all=pltpu.VMEM((3,) + blk + (width,), BF16), own=pltpu.VMEM((2, rows, width), BF16),
                part=pltpu.VMEM((HELD, 2 * rows, width), F32), give=pltpu.VMEM((nz, rows, width), BF16),
                pair=pltpu.VMEM((2, nz, rows, width), BF16), send=pltpu.VMEM((2, steps, size, width), BF16),
                recv=pltpu.VMEM((2, 2, steps, size, width), BF16),
                wqt_v=pltpu.VMEM((3 * e, width), BF16), wot_v=pltpu.VMEM((width, e), BF16),
                wut_v=pltpu.VMEM((f, width), BF16), wdt_v=pltpu.VMEM((width, f), BF16),
                q=pltpu.VMEM((n_layers,) + blk + (e,), BF16), k=pltpu.VMEM((n_layers,) + blk + (e,), BF16),
                v=pltpu.VMEM((n_layers,) + blk + (e,), BF16), attn=pltpu.VMEM((n_layers,) + blk + (e,), BF16),
                prob=pltpu.VMEM(blk + (seq,), BF16), pre=pltpu.VMEM(blk + (f,), F32),
                act=pltpu.VMEM((n_layers,) + blk + (f,), BF16),
                gs=dma((lands, 4, 2, far + 1, PIECES)), ss=dma((2, 2, 2, steps)), ps=dma((2, 2, nz)), local=dma((signals,)))

        def call(body, cid, inputs, outputs, scratch):
            names = list(inputs) + list(outputs) + list(scratch)

            def kernel(*refs):
                body(types.SimpleNamespace(**dict(zip(names, refs))), n, n_layers)

            out = pl.pallas_call(
                kernel, out_shape=[jax.ShapeDtypeStruct(shape, dtype) for shape, dtype, _ in outputs.values()],
                in_specs=[spec for _, spec in inputs.values()], out_specs=[spec for _, _, spec in outputs.values()],
                scratch_shapes=list(scratch.values()),
                compiler_params=pltpu.CompilerParams(collective_id=cid, has_side_effects=True, vmem_limit_bytes=67043328),
                name=body.__name__)(*[arr for arr, _ in inputs.values()])
            return types.SimpleNamespace(**dict(zip(outputs, out)))

        both = dict(dy=(dy_loc[0], VM), ln=(ln_par, VM))
        weights = dict(
            wq=(jnp.transpose(w_qkv[:, :, :, 0], (0, 2, 1, 3)), ANY),
            wo=(w_out[:, 0], ANY), wu=(w_up, ANY), wd=(w_down, ANY))
        fwd = call(
            forward_kernel, 1, dict(x=(x_loc[0], VM), bias=(bias_d, VM), bup=(b_up[:, None], VM), **both, **weights),
            dict(y=((rows, width), BF16, VM), **saved),
            dict(
                comm(3, 32), wq_v=pltpu.VMEM((width, 3 * e), BF16), wo_v=pltpu.VMEM((e, width), BF16),
                wu_v=pltpu.VMEM((width, f), BF16), wd_v=pltpu.VMEM((f, width), BF16)))
        bwd = call(
            backward_kernel, 2, dict(both, **{name: (getattr(fwd, name), spec) for name, (_, _, spec) in saved.items()}),
            dict(
                dx=((rows, width), BF16, VM), ln_grad=(ln_par.shape, F32, VM), bias_grad=(bias_d.shape, F32, VM),
                dwq=((n_layers, 3, width, e), BF16, ANY), dwo=((n_layers, e, width), BF16, ANY),
                dwu=(w_up.shape, BF16, ANY), d_bup=(b_up.shape, F32, VM), dwd=(w_down.shape, BF16, ANY)),
            dict(
                comm(2, 32), d_res=pltpu.VMEM((rows, width), F32), d_pre=pltpu.VMEM(blk + (f,), BF16),
                d_proj=pltpu.VMEM(blk + (3 * e,), BF16), d_k=pltpu.VMEM((seq, e), F32), d_v=pltpu.VMEM((seq, e), F32),
                bup_sum=pltpu.VMEM((1, f), F32), dwq_v=pltpu.VMEM((3, width, e), BF16), dwo_v=pltpu.VMEM((e, width), BF16),
                dwu_v=pltpu.VMEM((width, f), BF16), dwd_v=pltpu.VMEM((f, width), BF16),
                small_a=pltpu.VMEM((few, width), F32), small_b=pltpu.VMEM((8, width), F32),
                got_a=pltpu.VMEM((n, few, cols), F32), got_b=pltpu.VMEM((n, 8, cols), F32),
                sum_a=pltpu.VMEM((few, width), F32), sum_b=pltpu.VMEM((8, width), F32), es=dma((2, 4, n))))
        y, dx, ln_grad, bias_grad, dwq, dwo, dwu, d_bup, dwd = write_out(
            fwd.y, bwd.dx, bwd.ln_grad, bwd.bias_grad, bwd.dwq, bwd.dwo, bwd.dwu, bwd.d_bup, bwd.dwd)
        return (y[None], dx[None], ln_grad, bias_grad, jnp.transpose(dwq, (0, 2, 1, 3))[:, :, :, None], dwo[:, None], dwu, d_bup, dwd)

    in_specs = (P('dp', 'tp', None), P('dp', 'tp', None), P(None, None, None), P(None, None, None),
                P(None, None, None, 'tp', None), P(None, 'tp', None, None), P(None, None, 'tp'), P(None, 'tp'), P(None, 'tp', None))
    out_specs = (P('dp', 'tp', None), P('dp', 'tp', None), P('dp', None, None), P('dp', None, None),
                 P('dp', None, None, 'tp', None), P('dp', 'tp', None, None), P('dp', None, 'tp'), P('dp', 'tp'), P('dp', 'tp', None))
    return jax.shard_map(device_step, mesh=mesh, in_specs=in_specs, out_specs=out_specs, check_vma=False)
```

```python
import math
import types

import jax
import jax.numpy as jnp
from jax import lax
from jax.experimental import pallas as pl
from jax.experimental.pallas import tpu as pltpu
from jax.sharding import PartitionSpec as P

F32 = jnp.float32
BF16 = jnp.bfloat16
MESH = pl.DeviceIdType.MESH
VM = pl.BlockSpec(memory_space=pltpu.VMEM)
ANY = pl.BlockSpec(memory_space=pl.ANY)
PIECES = 4
HELD = 5
TILE = 256
FINAL = (2, 0, 3, 1)
GATHER = {1: ((2, 0, 3, 1), (2, 0, 3, 1)), -1: ((2, 0, 3, 1), (2, 3, 0, 1), (3, 2, 1, 0))}
GATHER_FAR = {1: (2, 0), -1: (3, 1)}
SCATTER_FAR = {1: (0, 1), -1: (2, 3)}
SCATTER = {1: (2, 3, 0, 1), -1: (0, 1, 2, 3)}
SCATTER_TWO = {1: (2, 3, 0, 1), -1: (0, 2, 1, 3)}


def side(d):
    return (1 - d) // 2


def remote(src, dst, send_sem, recv_sem, dev):
    return pltpu.make_async_remote_copy(src_ref=src, dst_ref=dst, send_sem=send_sem, recv_sem=recv_sem,
                                        device_id={'tp': dev}, device_id_type=MESH)


class Ring:
    def __init__(self, n):
        self.n = n
        self.nz = n // 2
        self.far = self.nz // 2
        self.me = lax.axis_index('tp')
        self.z = self.me // 2
        self.c = lax.rem(self.me, 2)
        self.sib = self.me + 1 - 2 * self.c
        self.next = {1: lax.rem(self.me + 2, n), -1: lax.rem(self.me + n - 2, n)}
        self.peers = [lax.rem(self.me + j, n) for j in range(n)]

    def chip(self, off):
        return lax.rem(self.z + (off + self.nz), self.nz)

    def enter(self, devices):
        bar = pltpu.get_barrier_semaphore()
        for dev in devices:
            pl.semaphore_signal(bar, inc=1, device_id={'tp': dev}, device_id_type=MESH)
        pl.semaphore_wait(bar, len(devices))


class Gather:
    def __init__(self, ring, own, land, sems):
        self.ring, self.own, self.land = ring, own, land
        self.sems = sems
        self.rows = own.shape[0]
        self.size = self.rows // PIECES

    def piece(self, off, core, q):
        return self.land.at[self.ring.chip(off), pl.ds(pl.multiple_of(core * self.rows + q * self.size, self.size), self.size)]

    def order(self, d, k):
        if k == self.ring.far - 1:
            return GATHER_FAR[d]
        return GATHER[d][min(k, len(GATHER[d]) - 1)]

    def forward(self, d, k, q):
        dst = self.piece(-d * k, self.ring.c, q)
        src = self.own.at[pl.ds(q * self.size, self.size)] if k == 0 else dst
        return remote(src, dst, self.sems[0].at[side(d), k, q], self.sems[1].at[side(d), k, q], self.ring.next[d])

    def arrival(self, d, k, q):
        ref = self.piece(-d * (k + 1), self.ring.c, q)
        return remote(ref, ref, self.sems[0].at[side(d), k, q], self.sems[1].at[side(d), k, q], self.ring.next[d])

    def pair(self, d, k, q, core):
        ref = self.piece(-d * (k + 1), core, q)
        return remote(ref, ref, self.sems[2].at[side(d), k, q], self.sems[3].at[side(d), k, q], self.ring.sib)

    def own_pair(self, q, core):
        far = self.ring.far
        return remote(self.own.at[pl.ds(q * self.size, self.size)], self.piece(0, core, q),
                      self.sems[2].at[0, far, q], self.sems[3].at[0, far, q], self.ring.sib)

    def launch(self, q):
        for d in (1, -1):
            self.forward(d, 0, q).start()
        self.own_pair(q, self.ring.c).start()

    def place_own(self):
        self.land[self.ring.z, pl.ds(pl.multiple_of(self.ring.c * self.rows, self.rows), self.rows)] = self.own[...]
        for q in range(PIECES):
            self.own_pair(q, 1 - self.ring.c).wait_recv()

    def hop(self, k):
        far = self.ring.far
        wait = {d: list(self.order(d, k + 1)) if k + 1 < far else [] for d in (1, -1)}
        have = {1: set(), -1: set()}
        for i in range(len(self.order(1, k))):
            for d in (1, -1):
                q = self.order(d, k)[i]
                self.arrival(d, k, q).wait_recv()
                have[d].add(q)
                while wait[d] and wait[d][0] in have[d]:
                    self.forward(d, k + 1, wait[d].pop(0)).start()
                self.pair(d, k, q, self.ring.c).start()

    def paired(self, k):
        for d in (1, -1):
            for q in self.order(d, k):
                self.pair(d, k, q, 1 - self.ring.c).wait_recv()

    def offs(self, k):
        return (k + 1, -(k + 1)) if k < self.ring.far - 1 else (self.ring.far,)

    def run(self, on_hop, middle):
        self.place_own()
        on_hop([self.ring.z], True)
        for k in range(self.ring.far):
            self.hop(k)
            if k == self.ring.far - 2:
                middle()
            self.paired(k)
            on_hop([self.ring.chip(o) for o in self.offs(k)], False)

    def settle(self):
        for d in (1, -1):
            for k in range(self.ring.far):
                for q in self.order(d, k):
                    self.forward(d, k, q).wait_send()
                    self.pair(d, k, q, self.ring.c).wait_send()
        for q in range(PIECES):
            self.own_pair(q, self.ring.c).wait_send()


class Scatter:
    def __init__(self, ring, part, give, pair, send, recv, sems):
        self.ring, self.part, self.give, self.pair_ref, self.send, self.recv = ring, part, give, pair, send, recv
        self.sems = sems
        self.rows = give.shape[1]
        self.size = self.rows // PIECES
        far = ring.far
        self.groups = [(far,)] + [(k, -k) for k in range(far - 1, 0, -1)] + [(0,)]
        self.offs = [off for group in self.groups for off in group]
        self.slots = {}
        for d in (1, -1):
            self.slots[d] = [(far, q) for q in SCATTER_FAR[d]]
            for k in range(far - 1, 0, -1):
                order = FINAL if k == 1 else SCATTER_TWO[d] if k == 2 else SCATTER[d]
                self.slots[d] += [(k, q) for q in order]
        self.steps = len(self.slots[1])
        self.paired = set()
        self.made = 0
        self.filled = 0

    def pair(self, j):
        return remote(self.give.at[j], self.pair_ref.at[j], self.sems[2].at[j], self.sems[3].at[j], self.ring.sib)

    def hop(self, d, s):
        i = side(d)
        return remote(self.send.at[i, s], self.recv.at[i, s], self.sems[0].at[i, s], self.sems[1].at[i, s], self.ring.next[d])

    def fill(self, make):
        group = self.groups[self.filled]
        vals = make([self.ring.chip(off) for off in group])
        theirs = pl.ds(pl.multiple_of((1 - self.ring.c) * self.rows, self.rows), self.rows)
        for i in range(len(group)):
            j = self.made
            self.part[j % HELD] = vals[2 * i * self.rows:2 * (i + 1) * self.rows]
            self.give[j] = self.part[j % HELD, theirs].astype(BF16)
            self.pair(j).start()
            self.made += 1
        self.filled += 1

    def base(self, j, q):
        if j not in self.paired:
            self.pair(j).wait_recv()
            self.paired.add(j)
        at = pl.multiple_of(self.ring.c * self.rows + q * self.size, self.size)
        return self.part[j % HELD, pl.ds(at, self.size)] + self.pair_ref[j, pl.ds(q * self.size, self.size)].astype(F32)

    def run(self, make, work=None, count=0):
        fill_after = [2 + PIECES * g for g in range(len(self.groups) - 2)]
        quiet = [1] + list(range(PIECES, self.steps - 1, PIECES))
        begun = 0
        self.fill(make)
        self.fill(make)
        for s in range(self.steps):
            for d in (1, -1):
                k, q = self.slots[d][s]
                val = self.base(self.offs.index(d * k if k < self.ring.far else self.ring.far), q)
                if (k + 1, q) in self.slots[d]:
                    t = self.slots[d].index((k + 1, q))
                    self.hop(d, t).wait_recv()
                    val = val + self.recv[side(d), t].astype(F32)
                self.send[side(d), s] = val.astype(BF16)
                self.hop(d, s).start()
            if s in fill_after:
                self.fill(make)
            elif s in quiet and begun < count:
                upto = begun + -(-(count - begun) // len([t for t in quiet if t >= s]))
                if upto - begun == 1:
                    work(begun)
                else:
                    pl.loop(begun, upto)(work)
                begun = upto

    def total(self, q):
        val = self.base(len(self.offs) - 1, q)
        for d in (1, -1):
            s = self.slots[d].index((1, q))
            self.hop(d, s).wait_recv()
            val = val + self.recv[side(d), s].astype(F32)
        return val

    def settle(self):
        for d in (1, -1):
            for s in range(self.steps):
                self.hop(d, s).wait_send()
        for j in range(len(self.offs)):
            self.pair(j).wait_send()


class Exchange:
    def __init__(self, ring, rows, got, out, sems):
        self.ring, self.rows, self.got, self.out = ring, rows, got, out
        self.sems = sems
        self.cols = rows.shape[1] // ring.n

    def block(self, ref, dev):
        return ref.at[:, pl.ds(pl.multiple_of(dev * self.cols, self.cols), self.cols)]

    def first(self, j):
        peer = self.ring.peers[j]
        return remote(self.block(self.rows, peer), self.got.at[j], self.sems[0].at[j], self.sems[1].at[j], peer)

    def second(self, j, dev):
        return remote(self.got.at[0], self.block(self.out, dev), self.sems[2].at[j], self.sems[3].at[j], self.ring.peers[j])

    def start(self):
        for j in range(1, self.ring.n):
            self.first(j).start()

    def add(self):
        mine = pl.ds(pl.multiple_of(self.ring.me * self.cols, self.cols), self.cols)
        acc = self.rows[:, mine]
        for j in range(1, self.ring.n):
            self.first(j).wait_recv()
            acc = acc + self.got[j]
        self.got[0] = acc
        self.out[:, mine] = acc
        for j in range(1, self.ring.n):
            self.second(j, self.ring.me).start()

    def finish(self):
        for j in range(1, self.ring.n):
            self.second(j, lax.rem(self.ring.me + self.ring.n - j, self.ring.n)).wait_recv()
        for j in range(1, self.ring.n):
            self.first(j).wait_send()
            self.second(j, self.ring.me).wait_send()


class Local:
    def __init__(self, sems):
        self.sems = sems
        self.used = 0

    def copies(self, *pairs):
        at = self.used
        self.used += len(pairs)

        def of(l):
            return [pltpu.make_async_copy(*pair(l), self.sems.at[at + i]) for i, pair in enumerate(pairs)]

        return types.SimpleNamespace(start=lambda l: [c.start() for c in of(l)], wait=lambda l: [c.wait() for c in of(l)])


def dot(a, b, ca=1, cb=0):
    return lax.dot_general(a, b, (((ca,), (cb,)), ((), ())), preferred_element_type=F32)


def layer_norm(row_vals, ln_gain, ln_shift):
    mean_val = jnp.mean(row_vals, axis=-1, keepdims=True)
    centered = row_vals - mean_val
    var_val = jnp.mean(centered * centered, axis=-1, keepdims=True)
    return centered * lax.rsqrt(var_val + 1e-5) * ln_gain + ln_shift


def layer_norm_back(d_out, row_vals, ln_gain):
    mean_val = jnp.mean(row_vals, axis=-1, keepdims=True)
    centered = row_vals - mean_val
    var_val = jnp.mean(centered * centered, axis=-1, keepdims=True)
    inv = lax.rsqrt(var_val + 1e-5)
    unit = centered * inv
    scaled = d_out * ln_gain
    pull = scaled - jnp.mean(scaled, axis=-1, keepdims=True) - unit * jnp.mean(scaled * unit, axis=-1, keepdims=True)
    return pull * inv, d_out * unit


GELU_C = math.sqrt(2.0 / math.pi)


def gelu(x):
    return x * (0.5 * (1.0 + jnp.tanh(GELU_C * (x + 0.044715 * (x * x * x)))))


def gelu_slope(x):
    t = jnp.tanh(GELU_C * (x + 0.044715 * (x * x * x)))
    return 0.5 * (1.0 + t) + 0.5 * x * (1.0 - t * t) * (GELU_C * (1.0 + 3 * 0.044715 * (x * x)))


def rows_of(ref, chips):
    parts = [ref[z] for z in chips]
    return parts[0] if len(parts) == 1 else jnp.concatenate(parts, axis=0)


def put_rows(ref, chips, vals):
    m = ref.shape[1]
    for i, z in enumerate(chips):
        ref[z] = vals[i * m:(i + 1) * m].astype(ref.dtype)


def put_turned(ref, chips, vals):
    m = vals.shape[0] // len(chips)
    for i, z in enumerate(chips):
        ref[:, pl.ds(pl.multiple_of(z * m, m), m)] = vals[i * m:(i + 1) * m].T


def flat(ref, cols=None):
    vals = ref[...] if cols is None else ref[:, :, cols]
    return vals.reshape(vals.shape[0] * vals.shape[1], vals.shape[2])


def col_sum(vals):
    return jnp.sum(vals, axis=0, keepdims=True)


def forward_kernel(r, n, n_layers):
    ring = Ring(n)
    local = Local(r.local)
    rows, width = r.dy.shape
    e = r.wq.shape[-1]
    size = rows // PIECES
    scale = e ** -0.5
    last = n_layers - 1
    gathers = [Gather(ring, own, r.all.at[i], [r.gs.at[i, t] for t in range(4)])
               for i, own in enumerate((r.own.at[0], r.own.at[1], r.dy))]

    def scatter_at(i):
        return Scatter(ring, r.part, r.give, r.pair.at[i], r.send, r.recv.at[i],
                       [r.ss.at[i, 0], r.ss.at[i, 1], r.ps.at[i, 0], r.ps.at[i, 1]])

    def piece(q):
        return pl.ds(q * size, size)

    attn_w = local.copies(*[lambda l, i=i: (r.wq.at[l, i], r.wq_v.at[:, pl.ds(i * e, e)]) for i in range(3)],
                          lambda l: (r.wo.at[l], r.wo_v))
    mlp_w = local.copies(lambda l: (r.wd.at[l], r.wd_v), lambda l: (r.wu.at[l], r.wu_v))
    dy = gathers[2]
    save_one = local.copies(*[lambda l, a=a, b=b: (a.at[l], b.at[l]) for a, b in ((r.q, r.q_h), (r.k, r.k_h), (r.v, r.v_h))])
    save_attn = local.copies(lambda l: (r.prob, r.prob_h.at[l]), lambda l: (r.attn_t, r.attn_h.at[l]), lambda l: (r.h_t, r.h_one.at[l]),
                             lambda l: (r.wqt_v, r.wqt.at[l]), lambda l: (r.wot_v, r.wot.at[l]))
    save_turn = local.copies(lambda l: (r.h_t, r.h_two.at[l]), lambda l: (r.wut_v, r.wut.at[l]), lambda l: (r.wdt_v, r.wdt.at[l]))
    save_mlp = local.copies(lambda l: (r.pre, r.pre_h.at[l]), lambda l: (r.act_t, r.act_h.at[l]))
    save_dy = local.copies(lambda l: (r.all.at[2], r.dy_all))

    attn_w.start(0)
    mlp_w.start(0)
    for q in FINAL:
        res = r.x[piece(q)].astype(F32)
        r.res[0, piece(q)] = res
        r.own[0, piece(q)] = layer_norm(res, r.ln[0, 0:1], r.ln[0, 1:2]).astype(BF16)
    ring.enter([ring.next[1], ring.next[-1], ring.sib])
    for q in FINAL:
        gathers[0].launch(q)

    def side_steps(phase, odd):
        for k in range(odd, min(2 * n_layers, ring.far), 2):
            @pl.when(phase == k)
            def _():
                if k == 0:
                    for q in FINAL:
                        dy.launch(q)
                else:
                    dy.hop(k - 1)

    @pl.loop(0, n_layers)
    def forward(l):
        inner = l < last

        def on_attn(chips, first):
            if first:
                attn_w.wait(l)
            vals = dot(rows_of(r.all.at[0], chips), r.wq_v[...]).astype(BF16)
            for i, ref in enumerate((r.q, r.k, r.v)):
                put_rows(ref.at[l], chips, vals[:, i * e:(i + 1) * e])

        def middle():
            side_steps(2 * l, 0)

            @pl.when(l > 0)
            def _():
                gathers[1].settle()
                scatter_at(1).settle()
                save_mlp.wait(l)
                save_turn.wait(l)

        gathers[0].run(on_attn, middle)
        save_one.start(l)

        def turn_attn(j):
            at = pl.ds(pl.multiple_of(j * TILE, TILE), TILE)
            r.wqt_v[:, at] = r.wq_v[at].T
            r.wot_v[at] = r.wo_v[:, at].T
            r.h_t[at] = flat(r.all.at[0], at).T

        def make(chips):
            s = dot(rows_of(r.q.at[l], chips), flat(r.k.at[l]), 1, 1) * scale
            one = lax.broadcasted_iota(jnp.int32, (2 * rows, s.shape[1]), 0)
            row = [one + z * (2 * rows) for z in chips]
            row = row[0] if len(row) == 1 else jnp.concatenate(row, axis=0)
            col = lax.broadcasted_iota(jnp.int32, s.shape, 1)
            s = jnp.where(row >= col, s, -1e30)
            s = jnp.exp(s - jnp.max(s, axis=-1, keepdims=True))
            p = (s / jnp.sum(s, axis=-1, keepdims=True)).astype(BF16)
            put_rows(r.prob, chips, p)
            a = dot(p, flat(r.v.at[l])).astype(BF16)
            put_turned(r.attn_t, chips, a)
            return dot(a, r.wo_v[...])

        sc = scatter_at(0)
        sc.run(make, turn_attn, width // TILE)
        for q in FINAL:
            res = r.res[2 * l, piece(q)] + sc.total(q) + r.bias[l, 0:1]
            r.res[2 * l + 1, piece(q)] = res
            r.own[1, piece(q)] = layer_norm(res, r.ln[l, 2:3], r.ln[l, 3:4]).astype(BF16)
            gathers[1].launch(q)
        save_attn.start(l)

        @pl.when(inner)
        def _():
            attn_w.start(l + 1)

        def on_mlp(chips, first):
            if first:
                mlp_w.wait(l)
            pre = dot(rows_of(r.all.at[1], chips), r.wu_v[...]) + r.bup[l]
            put_rows(r.pre, chips, pre)
            act = gelu(pre).astype(BF16)
            put_rows(r.act, chips, act)
            put_turned(r.act_t, chips, act)

        def middle_two():
            side_steps(2 * l + 1, 1)
            gathers[0].settle()
            scatter_at(0).settle()
            save_one.wait(l)
            save_attn.wait(l)

        gathers[1].run(on_mlp, middle_two)
        save_mlp.start(l)

        def turn_mlp(j):
            at = pl.ds(pl.multiple_of(j * TILE, TILE), TILE)
            r.wut_v[:, at] = r.wu_v[at].T
            r.wdt_v[at] = r.wd_v[:, at].T
            r.h_t[at] = flat(r.all.at[1], at).T

        sc = scatter_at(1)
        sc.run(lambda chips: dot(rows_of(r.act, chips), r.wd_v[...]), turn_mlp, width // TILE)
        save_turn.start(l)
        for q in FINAL:
            res = r.res[2 * l + 1, piece(q)] + sc.total(q) + r.bias[l, 1:2]
            r.y[piece(q)] = res.astype(BF16)

            @pl.when(inner)
            def _():
                r.res[2 * l + 2, piece(q)] = res
                r.own[0, piece(q)] = layer_norm(res, r.ln[l + 1, 0:1], r.ln[l + 1, 1:2]).astype(BF16)
                gathers[0].launch(q)

        @pl.when(inner)
        def _():
            mlp_w.start(l + 1)

    for k in range(min(2 * n_layers, ring.far) - 1, ring.far):
        dy.hop(k)
    dy.place_own()
    for k in range(ring.far):
        dy.paired(k)

    save_dy.start(0)
    dy.settle()
    gathers[1].settle()
    scatter_at(1).settle()
    save_mlp.wait(last)
    save_turn.wait(last)
    save_dy.wait(0)


def backward_kernel(r, n, n_layers):
    ring = Ring(n)
    local = Local(r.local)
    rows, width = r.dy.shape
    e = r.q.shape[-1]
    size = rows // PIECES
    scale = e ** -0.5
    last = n_layers - 1
    gathers = [Gather(ring, own, r.all.at[i], [r.gs.at[i, t] for t in range(4)])
               for i, own in enumerate((r.own.at[0], r.own.at[1]))]

    def scatter_at(i):
        return Scatter(ring, r.part, r.give, r.pair.at[i], r.send, r.recv.at[i],
                       [r.ss.at[i, 0], r.ss.at[i, 1], r.ps.at[i, 0], r.ps.at[i, 1]])

    def piece(q):
        return pl.ds(q * size, size)

    attn_w = local.copies(lambda l: (r.wot.at[l], r.wot_v), lambda l: (r.wqt.at[l], r.wqt_v))
    mlp_w = local.copies(lambda l: (r.wdt.at[l], r.wdt_v), lambda l: (r.wut.at[l], r.wut_v))
    blocks = width // TILE
    load_one = local.copies(lambda l: (r.h_one.at[l], r.h_t))
    load_two = local.copies(lambda l: (r.h_two.at[l], r.h_t))
    load_top = local.copies(lambda l: (r.dy_all, r.all.at[2]))
    load_prob = local.copies(lambda l: (r.prob_h.at[l], r.prob))
    load_pre = local.copies(lambda l: (r.pre_h.at[l], r.pre))
    load_act = local.copies(lambda l: (r.act_h, r.act_t))
    load_attn = local.copies(*[lambda l, a=a, b=b: (a, b) for a, b in
                               ((r.q_h, r.q), (r.k_h, r.k), (r.v_h, r.v), (r.attn_h, r.attn_t))])
    save_dmlp = local.copies(lambda l: (r.dwd_v, r.dwd.at[l]), lambda l: (r.dwu_v, r.dwu.at[l]))
    save_dattn = local.copies(lambda l: (r.dwo_v, r.dwo.at[l]), lambda l: (r.dwq_v, r.dwq.at[l]))

    load_top.start(0)
    load_pre.start(last)
    mlp_w.start(last)
    load_two.start(last)
    load_act.start(0)
    attn_w.start(last)
    load_prob.start(last)
    load_attn.start(0)
    for q in FINAL:
        r.d_res[piece(q)] = r.dy[piece(q)].astype(F32)
    r.small_a[...] = jnp.zeros_like(r.small_a)
    r.small_b[...] = jnp.zeros_like(r.small_b)
    ring.enter(ring.peers[1:])

    def put_small(l, i, val):
        for m in range(n_layers):
            @pl.when(l == m)
            def _():
                if m == 0 and i < 2:
                    r.small_b[i:i + 1] = val
                else:
                    at = i - 2 if m == 0 else 6 * m - 2 + i
                    r.small_a[at:at + 1] = val

    def backward_tail(sc, res_at, gain, after, out):
        d_gain = d_shift = d_bias = 0.0
        for q in FINAL:
            d_h = sc.total(q)
            d_in, terms = layer_norm_back(d_h, r.res[res_at, piece(q)], gain)
            d_new = r.d_res[piece(q)] + d_in
            out(q, d_new)
            d_gain, d_shift, d_bias = d_gain + col_sum(terms), d_shift + col_sum(d_h), d_bias + col_sum(d_new)
            r.d_res[piece(q)] = d_new
        after(d_gain, d_shift, d_bias)

    put_small(last, 5, col_sum(r.d_res[...]))
    ex_a = Exchange(ring, r.small_a, r.got_a, r.sum_a, [r.es.at[0, t] for t in range(4)])
    ex_b = Exchange(ring, r.small_b, r.got_b, r.sum_b, [r.es.at[1, t] for t in range(4)])

    @pl.loop(0, n_layers)
    def backward(i):
        l = last - i
        top, lower = i == 0, i > 0
        at_d = 1 + (n_layers - i) // n_layers

        @pl.when(lower)
        def _():
            load_two.start(l)
            load_prob.start(l)

        r.bup_sum[...] = jnp.zeros_like(r.bup_sum)

        def on_mlp(chips, first):
            if first:
                mlp_w.wait(l)
                load_pre.wait(l)
            d_act = dot(rows_of(r.all.at[at_d], chips), r.wdt_v[...])
            d_pre = d_act * gelu_slope(rows_of(r.pre, chips))
            r.bup_sum[...] += col_sum(d_pre)
            put_rows(r.d_pre, chips, d_pre)

        @pl.when(lower)
        def _():
            def middle():
                gathers[0].settle()
                scatter_at(1).settle()
                save_dattn.wait(l)
                load_two.wait(l)

            gathers[1].run(on_mlp, middle)

        @pl.when(top)
        def _():
            load_top.wait(0)
            load_pre.wait(l)
            mlp_w.wait(l)

            @pl.loop(0, ring.far)
            def _(z):
                on_mlp([z, z + ring.far], False)

            load_two.wait(l)
            load_act.wait(0)

        def mlp_work(j):
            cols = pl.ds(pl.multiple_of(j * TILE, TILE), TILE)
            r.dwd_v[:, cols] = dot(r.act_t[l], flat(r.all.at[at_d], cols)).astype(BF16)
            r.dwu_v[cols] = dot(r.h_t[cols], flat(r.d_pre)).astype(BF16)

        sc = scatter_at(0)
        sc.run(lambda chips: dot(rows_of(r.d_pre, chips), r.wut_v[...]), mlp_work, blocks)
        save_dmlp.start(l)

        def hand_on(q, d_new):
            r.own[0, piece(q)] = d_new.astype(BF16)
            gathers[0].launch(q)

        def after_mlp(d_gain, d_shift, d_bias):
            put_small(l, 2, d_gain)
            put_small(l, 3, d_shift)
            put_small(l, 4, d_bias)
            for m in range(n_layers):
                @pl.when(l == m)
                def _():
                    r.d_bup[m:m + 1] = r.bup_sum[...]

        backward_tail(sc, 2 * l + 1, r.ln[l, 2:3], after_mlp, hand_on)

        @pl.when(l > 0)
        def _():
            load_pre.start(l - 1)
            mlp_w.start(l - 1)

        @pl.when(l == 0)
        def _():
            ex_a.start()

        load_one.start(l)
        r.d_k[...] = jnp.zeros_like(r.d_k)
        r.d_v[...] = jnp.zeros_like(r.d_v)

        def on_attn(chips, first):
            if first:
                attn_w.wait(l)
                load_prob.wait(l)

                @pl.when(top)
                def _():
                    load_attn.wait(0)
            d_attn = dot(rows_of(r.all.at[0], chips), r.wot_v[...]).astype(BF16)
            prob = rows_of(r.prob, chips)
            d_prob = dot(d_attn, flat(r.v.at[l]), 1, 1)
            row_dot = jnp.sum(d_prob * prob, axis=-1, keepdims=True)
            d_score = (prob * (d_prob - row_dot) * scale).astype(BF16)
            d_q = dot(d_score, flat(r.k.at[l])).astype(BF16)
            for t, z in enumerate(chips):
                r.d_proj[z, :, 0:e] = d_q[t * 2 * rows:(t + 1) * 2 * rows]
            r.d_k[...] += dot(d_score, rows_of(r.q.at[l], chips), 0, 0)
            r.d_v[...] += dot(prob, d_attn, 0, 0)

        def middle_two():
            @pl.when(lower)
            def _():
                gathers[1].settle()

            scatter_at(0).settle()
            save_dmlp.wait(l)
            load_one.wait(l)

        gathers[0].run(on_attn, middle_two)
        blk = r.d_proj.shape[:2] + (e,)
        r.d_proj[:, :, e:2 * e] = r.d_k[...].astype(BF16).reshape(blk)
        r.d_proj[:, :, 2 * e:] = r.d_v[...].astype(BF16).reshape(blk)

        def attn_work(j):
            cols = pl.ds(pl.multiple_of(j * TILE, TILE), TILE)
            r.dwo_v[:, cols] = dot(r.attn_t[l], flat(r.all.at[0], cols)).astype(BF16)
            vals = dot(r.h_t[cols], flat(r.d_proj)).astype(BF16)
            for t in range(3):
                r.dwq_v[t, cols] = vals[:, t * e:(t + 1) * e]

        sc = scatter_at(1)
        sc.run(lambda chips: dot(rows_of(r.d_proj, chips), r.wqt_v[...]), attn_work, blocks)
        save_dattn.start(l)

        @pl.when(l == 0)
        def _():
            ex_a.add()

        def out(q, d_new):
            r.dx[piece(q)] = d_new.astype(BF16)

            @pl.when(l > 0)
            def _():
                r.own[1, piece(q)] = d_new.astype(BF16)
                gathers[1].launch(q)

        def after_attn(d_gain, d_shift, d_bias):
            put_small(l, 0, d_gain)
            put_small(l, 1, d_shift)
            put_small(l - 1, 5, d_bias)

        backward_tail(sc, 2 * l, r.ln[l, 0:1], after_attn, out)

        @pl.when(l > 0)
        def _():
            attn_w.start(l - 1)

    ex_b.start()
    gathers[0].settle()
    scatter_at(1).settle()
    ex_b.add()
    ex_a.finish()
    save_dattn.wait(0)
    ex_b.finish()
    for l in range(n_layers):
        for i in range(6):
            if l == 0 and i < 2:
                val = r.sum_b[i:i + 1]
            else:
                at = i - 2 if l == 0 else 6 * l - 2 + i
                val = r.sum_a[at:at + 1]
            if i < 4:
                r.ln_grad[l, i:i + 1] = val
            else:
                r.bias_grad[l, i - 4:i - 3] = val


def write_out(*results):
    parts = [(a, i) for a in sorted(range(len(results)), key=lambda a: -results[a].size)
             for i in (range(results[a].shape[0]) if results[a].ndim > 2 else [None])]

    def body(*refs):
        m = len(results)
        ins, outs, bufs, sems = refs[:m], refs[m:2 * m], refs[2 * m:3 * m], refs[3 * m]

        def at(ref, i):
            return ref if i is None else ref.at[i]

        reads = [pltpu.make_async_copy(at(ins[a], i), at(bufs[a], i), sems.at[0, t]) for t, (a, i) in enumerate(parts)]
        writes = [pltpu.make_async_copy(at(bufs[a], i), at(outs[a], i), sems.at[1, t]) for t, (a, i) in enumerate(parts)]
        for copy in reads:
            copy.start()
        for read, write in zip(reads, writes):
            read.wait()
            write.start()
        for write in writes:
            write.wait()

    return pl.pallas_call(
        body, out_shape=[jax.ShapeDtypeStruct(a.shape, a.dtype) for a in results], in_specs=[ANY] * len(results),
        out_specs=[ANY] * len(results),
        scratch_shapes=[pltpu.VMEM(a.shape, a.dtype) for a in results] + [pltpu.SemaphoreType.DMA((2, len(parts)))],
        compiler_params=pltpu.CompilerParams(vmem_limit_bytes=67043328), name='write_out')(*results)


def solution(mesh):
    n = mesh.shape['tp']

    def device_step(x_loc, dy_loc, ln_par, bias_d, w_qkv, w_out, w_up, b_up, w_down):
        n_layers = ln_par.shape[0]
        rows, width = x_loc.shape[1:]
        e, f = w_qkv.shape[-1], w_up.shape[-1]
        nz = n // 2
        far = nz // 2
        size = rows // PIECES
        steps = PIECES * (far - 1) + PIECES // 2
        blk = (nz, 2 * rows)
        seq = n * rows
        few = 8 * (-(-(6 * n_layers - 2) // 8))
        cols = width // n
        hbm = dict(
            h_one=((width, seq), BF16), h_two=((width, seq), BF16), pre_h=(blk + (f,), F32), act_h=((f, seq), BF16),
            prob_h=(blk + (seq,), BF16), q_h=(blk + (e,), BF16), k_h=(blk + (e,), BF16), v_h=(blk + (e,), BF16),
            attn_h=((e, seq), BF16),
            wqt=((3 * e, width), BF16), wot=((width, e), BF16), wut=((f, width), BF16), wdt=((width, f), BF16))
        saved = {name: ((n_layers,) + shape, dtype, ANY) for name, (shape, dtype) in hbm.items()}
        saved['dy_all'] = (blk + (width,), BF16, ANY)
        saved['res'] = ((2 * n_layers, rows, width), F32, VM)
        dma = pltpu.SemaphoreType.DMA

        def comm(lands, signals):
            return dict(
                all=pltpu.VMEM((3,) + blk + (width,), BF16), own=pltpu.VMEM((2, rows, width), BF16),
                part=pltpu.VMEM((HELD, 2 * rows, width), F32), give=pltpu.VMEM((nz, rows, width), BF16),
                pair=pltpu.VMEM((2, nz, rows, width), BF16), send=pltpu.VMEM((2, steps, size, width), BF16),
                recv=pltpu.VMEM((2, 2, steps, size, width), BF16),
                wqt_v=pltpu.VMEM((3 * e, width), BF16), wot_v=pltpu.VMEM((width, e), BF16),
                wut_v=pltpu.VMEM((f, width), BF16), wdt_v=pltpu.VMEM((width, f), BF16),
                q=pltpu.VMEM((n_layers,) + blk + (e,), BF16), k=pltpu.VMEM((n_layers,) + blk + (e,), BF16),
                v=pltpu.VMEM((n_layers,) + blk + (e,), BF16), h_t=pltpu.VMEM((width, seq), BF16),
                prob=pltpu.VMEM(blk + (seq,), BF16), pre=pltpu.VMEM(blk + (f,), F32),
                gs=dma((lands, 4, 2, far + 1, PIECES)), ss=dma((2, 2, 2, steps)), ps=dma((2, 2, nz)), local=dma((signals,)))

        def call(body, cid, inputs, outputs, scratch):
            names = list(inputs) + list(outputs) + list(scratch)

            def kernel(*refs):
                body(types.SimpleNamespace(**dict(zip(names, refs))), n, n_layers)

            out = pl.pallas_call(
                kernel, out_shape=[jax.ShapeDtypeStruct(shape, dtype) for shape, dtype, _ in outputs.values()],
                in_specs=[spec for _, spec in inputs.values()], out_specs=[spec for _, _, spec in outputs.values()],
                scratch_shapes=list(scratch.values()),
                compiler_params=pltpu.CompilerParams(collective_id=cid, has_side_effects=True, vmem_limit_bytes=67043328),
                name=body.__name__)(*[arr for arr, _ in inputs.values()])
            return types.SimpleNamespace(**dict(zip(outputs, out)))

        both = dict(dy=(dy_loc[0], VM), ln=(ln_par, VM))
        weights = dict(
            wq=(jnp.transpose(w_qkv[:, :, :, 0], (0, 2, 1, 3)), ANY),
            wo=(w_out[:, 0], ANY), wu=(w_up, ANY), wd=(w_down, ANY))
        fwd = call(
            forward_kernel, 1, dict(x=(x_loc[0], VM), bias=(bias_d, VM), bup=(b_up[:, None], VM), **both, **weights),
            dict(y=((rows, width), BF16, VM), **saved),
            dict(
                comm(3, 32), act=pltpu.VMEM(blk + (f,), BF16), act_t=pltpu.VMEM((f, seq), BF16), attn_t=pltpu.VMEM((e, seq), BF16),
                wq_v=pltpu.VMEM((width, 3 * e), BF16), wo_v=pltpu.VMEM((e, width), BF16),
                wu_v=pltpu.VMEM((width, f), BF16), wd_v=pltpu.VMEM((f, width), BF16)))
        bwd = call(
            backward_kernel, 2, dict(both, **{name: (getattr(fwd, name), spec) for name, (_, _, spec) in saved.items()}),
            dict(
                dx=((rows, width), BF16, VM), ln_grad=(ln_par.shape, F32, VM), bias_grad=(bias_d.shape, F32, VM),
                dwq=((n_layers, 3, width, e), BF16, ANY), dwo=((n_layers, e, width), BF16, ANY),
                dwu=(w_up.shape, BF16, ANY), d_bup=(b_up.shape, F32, VM), dwd=(w_down.shape, BF16, ANY)),
            dict(
                comm(2, 32), act_t=pltpu.VMEM((n_layers, f, seq), BF16), attn_t=pltpu.VMEM((n_layers, e, seq), BF16), d_res=pltpu.VMEM((rows, width), F32), d_pre=pltpu.VMEM(blk + (f,), BF16),
                d_proj=pltpu.VMEM(blk + (3 * e,), BF16), d_k=pltpu.VMEM((seq, e), F32), d_v=pltpu.VMEM((seq, e), F32),
                bup_sum=pltpu.VMEM((1, f), F32), dwq_v=pltpu.VMEM((3, width, e), BF16), dwo_v=pltpu.VMEM((e, width), BF16),
                dwu_v=pltpu.VMEM((width, f), BF16), dwd_v=pltpu.VMEM((f, width), BF16),
                small_a=pltpu.VMEM((few, width), F32), small_b=pltpu.VMEM((8, width), F32),
                got_a=pltpu.VMEM((n, few, cols), F32), got_b=pltpu.VMEM((n, 8, cols), F32),
                sum_a=pltpu.VMEM((few, width), F32), sum_b=pltpu.VMEM((8, width), F32), es=dma((2, 4, n))))
        y, dx, ln_grad, bias_grad, dwq, dwo, dwu, d_bup, dwd = write_out(
            fwd.y, bwd.dx, bwd.ln_grad, bwd.bias_grad, bwd.dwq, bwd.dwo, bwd.dwu, bwd.d_bup, bwd.dwd)
        return (y[None], dx[None], ln_grad, bias_grad, jnp.transpose(dwq, (0, 2, 1, 3))[:, :, :, None], dwo[:, None], dwu, d_bup, dwd)

    in_specs = (P('dp', 'tp', None), P('dp', 'tp', None), P(None, None, None), P(None, None, None),
                P(None, None, None, 'tp', None), P(None, 'tp', None, None), P(None, None, 'tp'), P(None, 'tp'), P(None, 'tp', None))
    out_specs = (P('dp', 'tp', None), P('dp', 'tp', None), P('dp', None, None), P('dp', None, None),
                 P('dp', None, None, 'tp', None), P('dp', 'tp', None, None), P('dp', None, 'tp'), P('dp', 'tp'), P('dp', 'tp', None))
    return jax.shard_map(device_step, mesh=mesh, in_specs=in_specs, out_specs=out_specs, check_vma=False)
```
